32 devices in a mesh: gx: 4 (over y, x), gy: 4 (over z), gz: 2 (over core).
Axes of the slice: x: 2, y: 2, z: 4, core: 2. Of those that a mesh axis runs over, the one named last changes fastest.
Arguments:
- old_data: float32 [384, 5, 16, 256], P(('gx', 'gy', 'gz')), may hold values from -6 to 24, as said below
- pair_old: int32 [256], P(('gx', 'gy', 'gz')), may hold values from 0 to 11
- pair_slot: int32 [256], P(('gx', 'gy', 'gz')), may hold values from 0 to 2
- pair_shift: int32 [256, 3], P(('gx', 'gy', 'gz')), may hold values from -2 to 2
- pair_dest: int32 [256, 1], P(('gx', 'gy', 'gz')), may hold values from 0 to 7; in each aligned block of 8 rows (0 to 7, 8 to 15, ...) at most 2 rows name the same one
- new_ratio: int32 [96], replicated, may hold values from 1 to 2, as said below
- neighbor_side: int32 [96, 6], P(('gx', 'gy', 'gz')), may hold values from 0 to 3
- neighbor_patch: int32 [96, 6], P(('gx', 'gy', 'gz')), may hold values from 0 to 2
Outputs:
- new_data: float32 [96, 5, 16, 256], P(('gx', 'gy', 'gz'))
- interface_jump: float32 [96, 5, 6, 256], P(('gx', 'gy', 'gz'))
- mass_totals: float32 [2, 5], replicated
The draws below stay inside these ranges and needn't reach their ends.
Inputs may be any that keep to these rules, and one draw needn't show every extreme that they name: `old_data`: values of order one whose level differs from patch to patch and field to field. `pair_dest`: on the rows of one device no owner is named more than 2 times, and some device names some owner exactly 2 times. `new_ratio`: 1 marks a new patch on the old level, 2 one coarser by a factor of two in each direction. `neighbor_side`: 0: on the device before in the order d, 1: on the same device, 2: on the device after, 3: no neighbour.
All inputs are finite; a program needn't handle non-finite values.
Results may differ from the reference program's by a relative error of at most 0.0001.
Values sent between devices are 32-bit elements; how exact they have to be, the bound alone decides.
A program may use at most 64 MiB of HBM per device.

```python
import math
import jax
import jax.numpy as jnp
import numpy as np
from jax import lax

FIELDS = 5
EDGE = 16
CAP = 2
P_OLD = 12
P_NEW = 3
PAIRS_DEV = 8
OLD = 384
NEW = 96
PAIRS = 256
N_GX = 4
N_GY = 4
N_GZ = 2
DEVICES = 32


def draw_old_data(key, part):
    noise_key, base_key = jax.random.split(key, 2)
    block_shape = (OLD, FIELDS, EDGE, EDGE * EDGE)
    rising = jnp.exp(jnp.log(3.0) * jnp.arange(OLD, dtype=jnp.float32) / max(OLD - 1, 1))
    field_base = jax.random.uniform(base_key, (FIELDS,), jnp.float32, 0.5, 2.0)
    noise_draw = jnp.clip(0.6 * jax.random.normal(noise_key, block_shape, jnp.float32), -2.0, 2.0)
    base_level = rising[:, None, None, None] * field_base[None, :, None, None]
    return (base_level * (1.0 + noise_draw)).astype(jnp.float32)


def draw_new_ratio(key, part):
    ratio_key = jax.random.fold_in(key, 17)
    picks = jax.random.randint(ratio_key, (NEW,), 0, 8, dtype=jnp.int32)
    return (1 + (picks == 0).astype(jnp.int32)).astype(jnp.int32)


def touch_ends(drawn, stream_key, smallest, largest):
    shape = drawn.shape
    place = [jax.random.randint(jax.random.fold_in(stream_key, axis), (), 0, shape[axis]) for axis in range(len(shape))]
    drawn = drawn.at[tuple(place)].set(smallest)
    longest = shape.index(max(shape))
    place[longest] = (place[longest] + 1) % shape[longest]
    return drawn.at[tuple(place)].set(largest)


def assign_block(own_key, own, number, rows, number_of, top, bound, slope):
    sequence = jax.random.permutation(own_key, number_of)
    crowded, ordinary = portions_of(number_of, rows * top, bound, slope, True), portions_of(number_of, rows * top, bound, slope, False)
    places = jnp.arange(number_of)

    def named(sizes, offset_by):
        used = int((sizes > 0).sum())
        fixed = max(1, used // 4)
        shifted = fixed + (places - fixed + offset_by * (used - fixed)) % max(1, number_of - fixed)
        return jnp.zeros((number_of,), jnp.int32).at[sequence[jnp.where(places < fixed, places, shifted)]].set(jnp.asarray(sizes, jnp.int32))

    sizes = jnp.where(number % 4 == 0, named(crowded, number // 4), named(ordinary, number - number // 4 - 1))
    mixed = jax.random.permutation(jax.random.fold_in(own, 3), number_of)
    donor, taker = mixed[0:number_of // 2 * 2:2], mixed[1:number_of // 2 * 2:2]
    slack = jnp.minimum(sizes[donor] - 1, bound - sizes[taker]) // 2
    slack = jnp.where((donor == sequence[0]) | (taker == sequence[0]) | (sizes[taker] == 0), 0, jnp.maximum(slack, 0))
    shifted = jax.random.randint(jax.random.fold_in(own, 4), (number_of // 2,), 0, 1 << 20) % (slack + 1)
    sizes = sizes.at[donor].add(-shifted).at[taker].add(shifted)
    labels = jnp.searchsorted(jnp.cumsum(sizes), jnp.arange(rows * top), side="right").astype(jnp.int32)
    grid = labels.reshape(top, rows).T
    grid = grid[jax.random.permutation(jax.random.fold_in(own, 1), rows)]
    offset_by = jax.random.randint(jax.random.fold_in(own, 2), (rows, 1), 0, top)
    return jnp.take_along_axis(grid, (jnp.arange(top)[None, :] + offset_by) % top, axis=1)


def portions_of(number_of, total, reach, skew, full):
    weights = [(1 << 20) // math.isqrt(standing ** skew) + 1 for standing in range(1, number_of + 1)]
    largest = reach if full else min(reach, max(-(-total // number_of), total * weights[0] // sum(weights)))
    least = 1 if total - largest >= number_of - 1 else 0
    holding, rest = [largest] + [least] * (number_of - 1), total - largest - least * (number_of - 1)
    while rest > 0:
        movable = [i for i in range(1, number_of) if holding[i] < largest] or [i for i in range(1, number_of) if holding[i] < reach]
        whole, left = sum([weights[i] for i in movable]), rest
        for i in movable:
            addition = min(reach - holding[i], max(1, left * weights[i] // whole), rest)
            holding[i] = holding[i] + addition
            rest = rest - addition
    return np.array(holding)


def setup_inputs(seed: int = 0) -> dict:
    key_list = jax.random.split(jax.random.key(seed), 9)
    old_data = draw_old_data(jax.random.fold_in(key_list[8], 71), 0)
    pair_old = touch_ends(jax.random.randint(key_list[1], (PAIRS,), 0, P_OLD), jax.random.fold_in(key_list[1], 1), 0, P_OLD - 1).astype(jnp.int32)
    pair_slot = touch_ends(jax.random.randint(key_list[2], (PAIRS,), 0, P_NEW), jax.random.fold_in(key_list[2], 1), 0, P_NEW - 1).astype(jnp.int32)
    pair_shift = touch_ends(jax.random.randint(key_list[3], (PAIRS, 3), -2, 3), jax.random.fold_in(key_list[3], 1), -2, 2).astype(jnp.int32)
    pair_dest_keys = jax.random.split(jax.random.fold_in(key_list[4], 1), PAIRS // PAIRS_DEV)
    pair_dest_turns = jax.random.permutation(jax.random.fold_in(key_list[4], 3), PAIRS // PAIRS_DEV)
    pair_dest = jax.vmap(lambda own, number: assign_block(jax.random.fold_in(key_list[4], 2), own, number, PAIRS_DEV, N_GX * N_GZ, 1, CAP, 2))(pair_dest_keys, pair_dest_turns).reshape((PAIRS, 1))
    new_ratio = draw_new_ratio(jax.random.fold_in(key_list[8], 71), 0)
    neighbor_side = touch_ends(jax.random.randint(key_list[6], (NEW, 6), 0, 4), jax.random.fold_in(key_list[6], 1), 0, 3).astype(jnp.int32)
    neighbor_patch = touch_ends(jax.random.randint(key_list[7], (NEW, 6), 0, P_NEW), jax.random.fold_in(key_list[7], 1), 0, P_NEW - 1).astype(jnp.int32)
    return dict(old_data=old_data, pair_old=pair_old, pair_slot=pair_slot, pair_shift=pair_shift, pair_dest=pair_dest, new_ratio=new_ratio, neighbor_side=neighbor_side, neighbor_patch=neighbor_patch)


precise = lax.Precision.HIGHEST


def intersection_weights(offsets, ratios, edge_cells):
    cell_index = jnp.arange(edge_cells, dtype=jnp.int32)
    distance = cell_index[None, None, :] - offsets[:, None, None]
    within = (distance >= 0) & (jnp.floor_divide(distance, ratios[:, None, None]) == cell_index[None, :, None])
    scaled = 1.0 / ratios[:, None, None].astype(jnp.float32)
    return jnp.where(within, scaled, jnp.zeros_like(scaled)).astype(jnp.float32)


def reference(old_data, pair_old, pair_slot, pair_shift, pair_dest, new_ratio, neighbor_side, neighbor_patch):
    pair_ids = jnp.arange(PAIRS, dtype=jnp.int32)
    sender = pair_ids // PAIRS_DEV
    sender_y = (sender // N_GZ) % N_GY
    target = pair_dest[:, 0]
    owner_device = ((target // N_GZ) * N_GY + sender_y) * N_GZ + target % N_GZ
    new_index = (owner_device * P_NEW + pair_slot).astype(jnp.int32)
    old_index = (sender * P_OLD + pair_old).astype(jnp.int32)
    ratios = new_ratio[new_index]
    block_size = math.gcd(PAIRS, 256)

    def add_block(block_index, totals):
        start = (block_index * block_size).astype(jnp.int32)
        sources = lax.dynamic_slice_in_dim(old_index, start, block_size)
        targets = lax.dynamic_slice_in_dim(new_index, start, block_size)
        shifts = lax.dynamic_slice_in_dim(pair_shift, start, block_size)
        block_ratio = lax.dynamic_slice_in_dim(ratios, start, block_size)
        cube_data = old_data[sources].reshape(block_size, FIELDS, EDGE, EDGE, EDGE)
        weight_x = intersection_weights(shifts[:, 0], block_ratio, EDGE)
        weight_y = intersection_weights(shifts[:, 1], block_ratio, EDGE)
        weight_z = intersection_weights(shifts[:, 2], block_ratio, EDGE)
        section_x = jnp.einsum("pim,pfmnl->pfinl", weight_x, cube_data, precision=precise)
        section_y = jnp.einsum("pjn,pfinl->pfijl", weight_y, section_x, precision=precise)
        section_z = jnp.einsum("pkl,pfijl->pfijk", weight_z, section_y, precision=precise)
        return totals.at[targets].add(section_z.reshape(block_size, FIELDS, EDGE, EDGE * EDGE))

    new_data = lax.fori_loop(0, PAIRS // block_size, add_block, jnp.zeros((NEW, FIELDS, EDGE, EDGE * EDGE), jnp.float32))

    cube_view = new_data.reshape(NEW, FIELDS, EDGE, EDGE, EDGE)
    face_layers = jnp.stack([cube_view[:, :, 0], cube_view[:, :, -1], cube_view[:, :, :, 0], cube_view[:, :, :, -1], cube_view[:, :, :, :, 0], cube_view[:, :, :, :, -1]], axis=2).reshape(NEW, FIELDS, 6, EDGE * EDGE)
    opposite = face_layers.reshape(NEW, FIELDS, 3, 2, EDGE * EDGE)[:, :, :, ::-1].reshape(NEW, FIELDS, 6, EDGE * EDGE)
    device_of = jnp.arange(NEW, dtype=jnp.int32) // P_NEW
    source_device = device_of[:, None] + neighbor_side - 1
    present = (neighbor_side < 3) & (source_device >= 0) & (source_device < DEVICES)
    neighbor_index = (jnp.clip(source_device, 0, DEVICES - 1) * P_NEW + neighbor_patch).astype(jnp.int32)
    by_face = jnp.transpose(opposite, (0, 2, 1, 3))
    ghosts = by_face[neighbor_index, jnp.arange(6, dtype=jnp.int32)[None, :]]
    ghosts = jnp.transpose(ghosts, (0, 2, 1, 3))
    jumps = ghosts - face_layers
    interface_jump = jnp.where(present[:, None, :, None], jumps, jnp.zeros_like(jumps))

    total_cells = OLD * EDGE ** 3
    old_total = jnp.sum(old_data, axis=(0, 2, 3))
    ratio_cubes = new_ratio.astype(jnp.float32) ** 3
    new_total = jnp.sum(ratio_cubes[:, None] * jnp.sum(new_data, axis=(2, 3)), axis=0)
    mass_totals = jnp.stack([old_total, new_total]) / total_cells
    return new_data, interface_jump, mass_totals
```

```python
import functools

import jax
import jax.numpy as jnp
from jax import lax
from jax.experimental import pallas as pl
from jax.experimental.pallas import tpu as pltpu
from jax.sharding import PartitionSpec as P

MESH = pl.DeviceIdType.MESH
AXES = ("gx", "gy", "gz")
TURN_STEP = 9


def split_two(value):
    high = value.astype(jnp.bfloat16)
    low = (value - high.astype(jnp.float32)).astype(jnp.bfloat16)
    return high, low


def dot(a, b):
    return jnp.dot(a, b, preferred_element_type=jnp.float32)


def iota(shape, axis):
    return lax.broadcasted_iota(jnp.int32, shape, axis)


def plan_of(bits, n_new):
    chips = 1 << bits
    orders = [list(range(bits)), list(reversed(range(bits)))]

    def sends(order, j):
        done = sum(1 << b for b in order[:j])
        xs = [x for x in range(chips) if (x >> order[j]) & 1 and not x & done]
        return sorted(xs, key=lambda x: -bin(x).count("1"))

    steps = []
    for j in range(bits):
        for pair in zip(*(sends(order, j) for order in orders)):
            fine = j == bits - 1 or pair[0] == chips - 1
            for s in range(n_new) if fine else [None]:
                for c in range(2):
                    steps.append((j, c, pair[c], s))
    return orders, steps


def kernel(
    dims,
    old_hbm,
    pair_old_hbm,
    pair_slot_hbm,
    pair_shift_hbm,
    pair_dest_hbm,
    new_ratio_hbm,
    side_hbm,
    patch_hbm,
    new_out,
    jump_out,
    mass_out,
    pair_old,
    pair_slot,
    pair_shift,
    pair_dest,
    new_ratio,
    side_ref,
    patch_ref,
    old,
    parts,
    mine,
    theirs,
    partner_in,
    chip_in,
    spread,
    faces,
    ghosts,
    mass_group,
    mass_line,
    old_sem,
    table_sem,
    turn,
    row_ready,
    far_ready,
    d2d_send,
    d2d_recv,
    chip_send,
    chip_recv,
    face_send,
    face_recv,
    group_send,
    group_recv,
    line_send,
    line_recv,
):
    size_x, size_y, size_z, n_old, n_new, n_pairs, fields, edge = dims
    face = edge * edge
    rows = fields * edge
    half = edge // 2
    group = size_x * size_z
    chips = group // 2
    bits = chips.bit_length() - 1
    devices = group * size_y
    ix, iy, iz = (lax.axis_index(a) for a in AXES)
    rank = ix * size_z + iz
    core = lax.rem(rank, 2)
    chip = lax.div(rank, 2)
    linear = (ix * size_y + iy) * size_z + iz

    def at_rank(g):
        return (lax.div(g, size_z), iy, lax.rem(g, size_z))

    def at_linear(d):
        return (
            lax.div(d, size_y * size_z),
            lax.rem(lax.div(d, size_z), size_y),
            lax.rem(d, size_z),
        )

    def chip_at(x):
        other = chip
        for b in range(bits):
            if (x >> b) & 1:
                other = other + (1 - 2 * lax.rem(lax.div(chip, 1 << b), 2)) * (1 << b)
        return other

    has_before = linear > 0
    has_after = linear < devices - 1
    partner = at_rank(chip * 2 + 1 - core)
    last_z = iz == size_z - 1
    first_z = iz == 0
    last_y = iy == size_y - 1
    first_y = iy == 0

    def signal(sem, device):
        pl.semaphore_signal(sem, inc=1, device_id=device, device_id_type=MESH)

    old_copy = pltpu.make_async_copy(old_hbm, old, old_sem)
    old_copy.start()
    tables = (
        (pair_dest_hbm, pair_dest),
        (pair_slot_hbm, pair_slot),
        (new_ratio_hbm, new_ratio),
        (pair_old_hbm, pair_old),
        (pair_shift_hbm, pair_shift),
        (side_hbm, side_ref),
        (patch_hbm, patch_ref),
    )
    tables = [
        pltpu.make_async_copy(source, table, table_sem.at[i])
        for i, (source, table) in enumerate(tables)
    ]
    for table in tables:
        table.start()

    barrier = pltpu.get_barrier_semaphore()
    signal(barrier, partner)

    @pl.loop(2 * chip + 2, group)
    def _(r):
        signal(barrier, at_rank(r))

    @pl.loop(iy + 1, size_y)
    def _(y):
        signal(barrier, (ix, y, iz))

    up = last_z & (iy < size_y - 1)
    down = first_z & (iy > 0)
    turn_after = last_z & last_y & has_after
    turn_before = first_z & first_y & has_before

    @pl.when(up)
    def _():
        signal(barrier, at_linear(linear + 1))

    @pl.when(turn_before)
    def _():
        signal(barrier, at_linear(linear - 1))

    count = 1 + 2 * chip + iy + down.astype(jnp.int32) + turn_after.astype(jnp.int32)
    pl.semaphore_wait(barrier, count)

    @pl.loop(0, 2 * chip)
    def _(r):
        signal(row_ready, at_rank(r))

    @pl.loop(0, iy)
    def _(y):
        signal(far_ready, (ix, y, iz))

    @pl.when(down)
    def _():
        signal(far_ready, at_linear(linear - 1))

    @pl.when(turn_after)
    def _():
        signal(far_ready, at_linear(linear + 1))

    col = iota((face, face), 1)
    row = iota((face, face), 0)
    low_col = lax.rem(col, edge)
    for i, wanted in enumerate(
        (low_col, low_col + face - edge, low_col * edge, low_col * edge + edge - 1)
    ):
        spread[:, i * face : (i + 1) * face] = jnp.where(row == wanted, 1.0, 0.0).astype(
            jnp.bfloat16
        )

    @pl.when(jnp.logical_not(has_before))
    def _():
        ghosts[0:n_new] = jnp.zeros((n_new, *ghosts.shape[1:]), jnp.float32)

    @pl.when(jnp.logical_not(has_after))
    def _():
        ghosts[2 * n_new :] = jnp.zeros((n_new, *ghosts.shape[1:]), jnp.float32)

    for table in tables:
        table.wait()
    keys, ratios = [], []
    for p in range(n_pairs):
        target = pair_dest[p]
        owner = (lax.div(target, size_z) * size_y + iy) * size_z + lax.rem(target, size_z)
        keys.append(target * n_new + pair_slot[p])
        ratios.append(new_ratio[owner * n_new + pair_slot[p]])

    parts[n_pairs] = jnp.zeros(parts.shape[1:], jnp.float32)
    row_y = lax.div(row, edge)
    row_z = lax.rem(row, edge)
    l_row = iota((rows, 2 * rows), 0)
    l_col = iota((rows, 2 * rows), 1)
    l_col = jnp.where(l_col >= rows, l_col - rows, l_col)
    same_field = lax.div(l_row, edge) == lax.div(l_col, edge)
    l_i = lax.rem(l_row, edge)
    l_m = lax.rem(l_col, edge)

    old_copy.wait()

    old_acc = [jnp.zeros((8, face), jnp.float32) for _ in range(fields)]
    for o in range(n_old):
        for f in range(fields):
            for h in range(edge // 8):
                old_acc[f] = old_acc[f] + old[o, f, h * 8 : (h + 1) * 8, :]

    new_acc = [jnp.zeros((8, face), jnp.float32) for _ in range(fields)]
    for p in range(n_pairs):
        ratio = ratios[p]
        coarse = ratio == 2
        step = ratio - 1
        tx, ty, tz = pair_shift[0, p], pair_shift[1, p], pair_shift[2, p]
        scale = jnp.where(coarse, jnp.float32(0.125), jnp.float32(1.0))
        cube = jnp.where(coarse, jnp.float32(8.0), jnp.float32(1.0))
        block = old[pair_old[p]].reshape(rows, face)
        lx = (lax.shift_right_arithmetic(l_m - tx, jnp.full_like(l_m, step)) == l_i) & same_field
        lx = jnp.where(lx, 1.0, 0.0).astype(jnp.bfloat16)
        high, low = split_two(block)
        mixed = dot(lx, jnp.concatenate([high, low], axis=0))
        ky = lax.shift_right_arithmetic(row_y - ty, jnp.full_like(row, step))
        kz = lax.shift_right_arithmetic(row_z - tz, jnp.full_like(row, step))
        code = jnp.where((kz >= 0) & (kz < edge), ky * edge + kz, -1)
        weight = jnp.where(code == col, scale, jnp.float32(0.0)).astype(jnp.bfloat16)
        high, low = split_two(mixed)
        out = dot(high, weight) + dot(low, weight)
        for f in range(fields):
            for c in range(2):
                piece = out[f * edge + c * half : f * edge + (c + 1) * half]
                parts[p, c, f] = piece
                new_acc[f] = new_acc[f] + cube * piece

    def owner_sum(dst, x, s, core_of):
        target = chip_at(x) * 2 + core_of
        wanted = target * n_new + s
        first = jnp.int32(n_pairs)
        second = jnp.int32(n_pairs)
        for p in reversed(range(n_pairs)):
            hit = keys[p] == wanted
            second = jnp.where(hit, first, second)
            first = jnp.where(hit, jnp.int32(p), first)
        dst[x, :, s] = parts[first] + parts[second]

    orders, steps = plan_of(bits, n_new)

    def d2d_key(x, s):
        return (x, s) if x == chips - 1 else (x, None)

    d2d_order = []
    for _, _, x, s in steps:
        for t in range(n_new) if s is None else [s]:
            if d2d_key(x, t) not in d2d_order:
                d2d_order.append(d2d_key(x, t))
    d2d_order.append((0, None))

    def to_partner(key):
        x, s = key
        at = (x, slice(None), s) if s is not None else (x,)
        return pltpu.make_async_remote_copy(
            src_ref=theirs.at[at],
            dst_ref=partner_in.at[at],
            send_sem=d2d_send,
            recv_sem=d2d_recv.at[d2d_order.index(key)],
            device_id=partner,
            device_id_type=MESH,
        )

    for x, s in d2d_order:
        for t in range(n_new) if s is None else [s]:
            owner_sum(theirs, x, t, 1 - core)
        to_partner((x, s)).start()

    for x, s in d2d_order:
        for t in range(n_new) if s is None else [s]:
            owner_sum(mine, x, t, core)

    m_row = iota((16, 128), 0)
    m_col = iota((16, 128), 1)
    zero_rows = jnp.zeros((8 - fields, 128), jnp.float32)

    def lines(accs):
        out = [
            jnp.sum(a[:, :128] + a[:, 128:], axis=0, keepdims=True) for a in accs
        ]
        return out + [zero_rows]

    sums = jnp.concatenate(lines(old_acc) + lines(new_acc), axis=0)
    sums = jnp.sum(sums, axis=1, keepdims=True)
    sums = jnp.where(m_row == m_col, jnp.broadcast_to(sums, (16, 128)), 0.0)
    mass_group[0] = jnp.sum(sums, axis=0, keepdims=True)

    landed, joined = set(), set()

    def prepare(x, s):
        key = d2d_key(x, s)
        if key not in landed:
            landed.add(key)
            to_partner(key).wait_recv()
        if (x, s) not in joined:
            joined.add((x, s))
            mine[x, :, s] = mine[x, :, s] + partner_in[x, :, s]

    def to_chip(step):
        j, c, x, s = step
        here = (x, c) if s is None else (x, c, s)
        there = (x - 1, c) if s is None else (x - 1, c, s)
        return pltpu.make_async_remote_copy(
            src_ref=mine.at[here],
            dst_ref=chip_in.at[there],
            send_sem=chip_send,
            recv_sem=chip_recv.at[steps.index(step)],
            device_id=at_rank(chip_at(1 << orders[c][j]) * 2 + core),
            device_id_type=MESH,
        )

    waited = set()

    def take(c, x, s, j):
        total = mine[x, c, s]
        for b in orders[c][:j]:
            y = x | (1 << b)
            step = next(t for t in steps if t[1:3] == (c, y) and t[3] in (None, s))
            if step not in waited:
                waited.add(step)
                to_chip(step).wait_recv()
            total = total + chip_in[y - 1, c, s]
        return total

    leads = (core == 0) == (2 * iy < size_y)
    prepare(steps[0][2], 0)

    above = group - 2 * (chip + 1)

    @pl.when(above > 0)
    def _():
        pl.semaphore_wait(row_ready, above)

    def to_group(k):
        return pltpu.make_async_remote_copy(
            src_ref=mass_group.at[0],
            dst_ref=mass_group.at[k],
            send_sem=group_send,
            recv_sem=group_recv,
            device_id=at_rank(lax.rem(rank + k, group)),
            device_id_type=MESH,
        )

    for k in range(1, group):
        to_group(k).start()

    @pl.when(jnp.logical_not(leads))
    def _():
        pl.semaphore_wait(turn, 1)

    for n, step in enumerate(steps):
        j, c, x, s = step
        for t in range(n_new) if s is None else [s]:
            prepare(x, t)
            if j:
                mine[x, c, t] = take(c, x, t, j)
        to_chip(step).start()
        if n == TURN_STEP:

            @pl.when(leads)
            def _():
                signal(turn, partner)

    for s in range(n_new):
        prepare(0, s)

    def all_of(ref, send_sem, recv_sem):
        return pltpu.make_async_remote_copy(
            src_ref=ref,
            dst_ref=ref,
            send_sem=send_sem,
            recv_sem=recv_sem,
            device_id=partner,
            device_id_type=MESH,
        )

    every_group = all_of(mass_group.at[1:], group_send, group_recv)
    every_group.wait_recv()
    total = jnp.zeros(mass_group.shape[1:], jnp.float32)
    for a in range(group):
        total = total + mass_group[lax.rem(rank - a + group, group)]
    mass_line[0] = total

    beyond = size_y - 1 - iy + up.astype(jnp.int32) + turn_before.astype(jnp.int32)

    @pl.when(beyond > 0)
    def _():
        pl.semaphore_wait(far_ready, beyond)

    for k in range(1, size_y):
        pltpu.make_async_remote_copy(
            src_ref=mass_line.at[0],
            dst_ref=mass_line.at[k],
            send_sem=line_send,
            recv_sem=line_recv,
            device_id=(ix, lax.rem(iy + k, size_y), iz),
            device_id_type=MESH,
        ).start()
    every_line = all_of(mass_line.at[1:], line_send, line_recv)

    used = 6 * fields
    tall = faces.shape[1]
    f_row = iota((tall, 2 * rows), 0)
    f_col = iota((tall, 2 * rows), 1)
    f_col = jnp.where(f_col >= rows, f_col - rows, f_col)
    picks = (lax.div(f_row, 6) == lax.div(f_col, edge)) & (f_row < used)
    f_x = lax.rem(f_col, edge)
    gather = jnp.where(picks, 1.0, 0.0).astype(jnp.bfloat16)
    ends = [
        jnp.where(picks & (f_x == at), 1.0, 0.0).astype(jnp.bfloat16) for at in (0, edge - 1)
    ]
    u_row = iota((2 * rows, face), 0)
    u_col = iota((2 * rows, face), 1)
    diagonal = lax.rem(u_row, edge) == lax.div(u_col, edge)
    diagonal = jnp.concatenate([diagonal] * 4, axis=1)
    which = lax.rem(iota((tall, face), 0), 6)

    def face_copy(way, s):
        from_at, to_at = pl.ds(n_new, n_new), pl.ds(0 if way else 2 * n_new, n_new)
        if s is not None:
            from_at, to_at = n_new + s, s if way else 2 * n_new + s
        return pltpu.make_async_remote_copy(
            src_ref=ghosts.at[from_at],
            dst_ref=ghosts.at[to_at],
            send_sem=face_send.at[way],
            recv_sem=face_recv.at[way],
            device_id=at_linear(linear + 1 if way else linear - 1),
            device_id_type=MESH,
        )


    for s in range(n_new):
        for c in range(2):
            total = take(c, 0, s, bits)
            for f in range(fields):
                new_out[s, f, c * half : (c + 1) * half, :] = total[f]
        high, low = split_two(new_out[s].reshape(rows, face))
        both = jnp.concatenate([high, low], axis=0)
        wide = dot(both, spread[...])
        wide = jnp.where(diagonal, wide, 0.0).astype(jnp.bfloat16)
        sides = dot(gather, wide)
        layers = [dot(ends[0], both), dot(ends[1], both)]
        layers += [sides[:, i * face : (i + 1) * face] for i in range(4)]
        own = layers[0]
        swapped = layers[1]
        for e in range(1, 6):
            own = jnp.where(which == e, layers[e], own)
            swapped = jnp.where(which == e, layers[e ^ 1], swapped)
        faces[s] = own
        ghosts[n_new + s] = swapped

        @pl.when(has_after)
        def _(s=s):
            face_copy(1, s).start()

        @pl.when(has_before)
        def _(s=s):
            face_copy(0, s).start()

    every_line.wait_recv()
    total = jnp.zeros(mass_group.shape[1:], jnp.float32)
    for a in range(size_y):
        total = total + mass_line[lax.rem(iy - a + size_y, size_y)]
    total = total / float(n_old * devices * edge * face)
    for a in range(2):
        mass_out[a : a + 1, :] = total[:, 8 * a : 8 * a + fields]

    all_of(theirs, d2d_send, d2d_recv.at[0]).wait_send()
    all_of(chip_in, chip_send, chip_recv.at[0]).wait_send()
    every_group.wait_send()
    every_line.wait_send()

    @pl.when(has_before)
    def _():
        face_copy(1, None).wait_recv()
        face_copy(0, None).wait_send()

    @pl.when(has_after)
    def _():
        face_copy(0, None).wait_recv()
        face_copy(1, None).wait_send()

    for s in range(n_new):
        ghost = jnp.zeros((tall, face), jnp.float32)
        present = jnp.zeros((tall, face), jnp.int32)
        for e in range(6):
            side = side_ref[s, e]
            source = linear + side - 1
            here = (side < 3) & (source >= 0) & (source < devices)
            place = jnp.where(side < 3, side, 0) * n_new + patch_ref[s, e]
            ghost = jnp.where(which == e, ghosts[place], ghost)
            present = jnp.where(which == e, here.astype(jnp.int32), present)
        jump = jnp.where(present > 0, ghost - faces[s], 0.0)
        for f in range(fields):
            jump_out[s, f] = jump[6 * f : 6 * f + 6]


def write_out(*refs):
    sems = refs[-1]
    copies = [pltpu.make_async_copy(refs[i], refs[3 + i], sems.at[i]) for i in range(3)]
    for copy in copies:
        copy.start()
    for copy in copies:
        copy.wait()


def body(
    old_data, pair_old, pair_slot, pair_shift, pair_dest, new_ratio, neighbor_side, neighbor_patch
):
    n_old, fields, edge, face = old_data.shape
    n_pairs = pair_old.shape[0]
    n_new = neighbor_side.shape[0]
    size_x, size_y, size_z = (lax.axis_size(a) for a in AXES)
    group = size_x * size_z
    chips = group // 2
    assert size_z % 2 == 0 and chips & (chips - 1) == 0
    half = edge // 2
    bits = chips.bit_length() - 1
    tall = -(-6 * fields // 8) * 8
    dims = (size_x, size_y, size_z, n_old, n_new, n_pairs, fields, edge)
    f32 = jnp.float32
    vmem = pl.BlockSpec(memory_space=pltpu.VMEM)
    tables = (pair_old, pair_slot, pair_shift.T, pair_dest.reshape(n_pairs))
    tables += (new_ratio, neighbor_side, neighbor_patch)
    dma = pltpu.SemaphoreType.DMA
    shapes = ((n_new, fields, edge, face), (n_new, fields, 6, face), (2, fields))
    results = pl.pallas_call(
        functools.partial(kernel, dims),
        out_shape=tuple(pltpu.VMEM(s, f32) for s in shapes),
        in_specs=[pl.BlockSpec(memory_space=pl.ANY)] * 8,
        out_specs=(vmem, vmem, vmem),
        scratch_shapes=[pltpu.SMEM(t.shape, jnp.int32) for t in tables]
        + [
            pltpu.VMEM((n_old, fields, edge, face), f32),
            pltpu.VMEM((n_pairs + 1, 2, fields, half, face), f32),
            pltpu.VMEM((chips, 2, n_new, fields, half, face), f32),
            pltpu.VMEM((chips, 2, n_new, fields, half, face), f32),
            pltpu.VMEM((chips, 2, n_new, fields, half, face), f32),
            pltpu.VMEM((chips - 1, 2, n_new, fields, half, face), f32),
            pltpu.VMEM((face, 4 * face), jnp.bfloat16),
            pltpu.VMEM((n_new, tall, face), f32),
            pltpu.VMEM((3 * n_new, tall, face), f32),
            pltpu.VMEM((group, 1, 128), f32),
            pltpu.VMEM((size_y, 1, 128), f32),
            dma,
            dma((len(tables),)),
            pltpu.SemaphoreType.REGULAR,
            pltpu.SemaphoreType.REGULAR,
            pltpu.SemaphoreType.REGULAR,
            dma,
            dma((n_new + chips - 1,)),
            dma,
            dma((len(plan_of(bits, n_new)[1]),)),
            dma((2,)),
            dma((2,)),
            dma,
            dma,
            dma,
            dma,
        ],
        compiler_params=pltpu.CompilerParams(collective_id=0, has_side_effects=True),
    )(old_data, *tables)
    return pl.pallas_call(
        write_out,
        out_shape=tuple(jax.ShapeDtypeStruct(s, f32) for s in shapes),
        in_specs=[vmem] * 3,
        out_specs=(pl.BlockSpec(memory_space=pl.ANY),) * 3,
        scratch_shapes=[dma((3,))],
    )(*(pltpu.with_memory_space_constraint(r, pltpu.VMEM) for r in results))


def solution(mesh):
    whole = P(AXES)
    return jax.shard_map(
        body,
        mesh=mesh,
        in_specs=(whole, whole, whole, whole, whole, P(), whole, whole),
        out_specs=(whole, whole, P()),
        check_vma=False,
    )
```

```python
import functools

import jax
import jax.numpy as jnp
from jax import lax
from jax.experimental import pallas as pl
from jax.experimental.pallas import tpu as pltpu
from jax.sharding import PartitionSpec as P

MESH = pl.DeviceIdType.MESH
AXES = ("gx", "gy", "gz")
TURN_AT = 2
TURN_LAST = 1
EARLY_X1 = True
LEAD_MODE = 1


def split_two(value):
    high = value.astype(jnp.bfloat16)
    low = (value - high.astype(jnp.float32)).astype(jnp.bfloat16)
    return high, low


def dot(a, b):
    return jnp.dot(a, b, preferred_element_type=jnp.float32)


def iota(shape, axis):
    return lax.broadcasted_iota(jnp.int32, shape, axis)


def plan_of(bits, n_new):
    chips = 1 << bits
    orders = [list(range(bits)), list(reversed(range(bits)))]

    def sends(order, j):
        done = sum(1 << b for b in order[:j])
        xs = [x for x in range(chips) if (x >> order[j]) & 1 and not x & done]
        return sorted(xs, key=lambda x: -bin(x).count("1"))

    steps = []
    for j in range(bits):
        for pair in zip(*(sends(order, j) for order in orders)):
            fine = j == bits - 1 or pair[0] == chips - 1
            for s in range(n_new) if fine else [None]:
                for c in range(2):
                    steps.append((j, c, pair[c], s))
    return orders, steps


def kernel(
    dims,
    old_hbm,
    pair_old_hbm,
    pair_slot_hbm,
    pair_shift_hbm,
    pair_dest_hbm,
    new_ratio_hbm,
    side_hbm,
    patch_hbm,
    new_out,
    jump_out,
    mass_out,
    pair_old,
    pair_slot,
    pair_shift,
    pair_dest,
    new_ratio,
    side_ref,
    patch_ref,
    gap,
    near_x,
    old,
    parts,
    mine,
    theirs,
    partner_in,
    chip_in,
    faces,
    ghosts,
    mass_own,
    mass_in,
    mass_line,
    old_sem,
    table_sem,
    turn,
    near,
    far_ready,
    d2d_send,
    d2d_recv,
    chip_send,
    chip_recv,
    face_send,
    face_recv,
    mass_send,
    mass_recv,
    line_send,
    line_recv,
):
    size_x, size_y, size_z, n_old, n_new, n_pairs, fields, edge = dims
    face = edge * edge
    rows = fields * edge
    half = edge // 2
    group = size_x * size_z
    chips = group // 2
    bits = chips.bit_length() - 1
    devices = group * size_y
    ix, iy, iz = (lax.axis_index(a) for a in AXES)
    rank = ix * size_z + iz
    core = lax.rem(rank, 2)
    chip = lax.div(rank, 2)
    linear = (ix * size_y + iy) * size_z + iz

    def at_rank(g):
        return (lax.div(g, size_z), iy, lax.rem(g, size_z))

    def at_linear(d):
        return (
            lax.div(d, size_y * size_z),
            lax.rem(lax.div(d, size_z), size_y),
            lax.rem(d, size_z),
        )

    def chip_at(x):
        other = chip
        for b in range(bits):
            if (x >> b) & 1:
                other = other + (1 - 2 * lax.rem(lax.div(chip, 1 << b), 2)) * (1 << b)
        return other

    has_before = linear > 0
    has_after = linear < devices - 1
    partner = at_rank(chip * 2 + 1 - core)
    last_z = iz == size_z - 1
    first_z = iz == 0
    last_y = iy == size_y - 1
    first_y = iy == 0

    def signal(sem, device):
        pl.semaphore_signal(sem, inc=1, device_id=device, device_id_type=MESH)

    old_copy = pltpu.make_async_copy(old_hbm, old, old_sem)
    old_copy.start()
    tables = (
        (pair_dest_hbm, pair_dest),
        (pair_slot_hbm, pair_slot),
        (new_ratio_hbm, new_ratio),
        (pair_old_hbm, pair_old),
        (pair_shift_hbm, pair_shift),
        (side_hbm, side_ref),
        (patch_hbm, patch_ref),
    )
    tables = [
        pltpu.make_async_copy(source, table, table_sem.at[i])
        for i, (source, table) in enumerate(tables)
    ]
    for table in tables:
        table.start()

    def bit(b):
        return lax.rem(lax.div(chip, 1 << b), 2)

    def near_chip(b):
        return at_rank(chip_at(1 << b) * 2 + core)

    end = last_z & last_y
    start = first_z & first_y
    up = (core == 1) & has_after & jnp.logical_not(end)
    down = (core == 0) & has_before & jnp.logical_not(start)
    turn_after = end & has_after
    turn_before = start & has_before

    barrier = pltpu.get_barrier_semaphore()
    signal(barrier, partner)
    for b in range(bits):

        @pl.when(bit(b) == 0)
        def _(b=b):
            signal(barrier, near_chip(b))

    @pl.loop(iy + 1, size_y)
    def _(y):
        signal(barrier, (ix, y, iz))

    @pl.when(up)
    def _():
        signal(barrier, at_linear(linear + 1))

    @pl.when(turn_before)
    def _():
        signal(barrier, at_linear(linear - 1))

    count = 1 + iy + down.astype(jnp.int32) + turn_after.astype(jnp.int32)
    for b in range(bits):
        count = count + bit(b)

    def greet():
        pl.semaphore_wait(barrier, count)
        for b in range(bits):

            @pl.when(bit(b) == 1)
            def _(b=b):
                signal(near.at[b], near_chip(b))

        @pl.loop(0, iy)
        def _(y):
            signal(far_ready, (ix, y, iz))

        @pl.when(down)
        def _():
            signal(far_ready, at_linear(linear - 1))

        @pl.when(turn_after)
        def _():
            signal(far_ready, at_linear(linear + 1))

    pl.when(jnp.logical_not(turn_after))(greet)

    col = iota((face, face), 1)
    row = iota((face, face), 0)
    for s in range(n_new):
        ghosts[n_new + s] = jnp.zeros(ghosts.shape[1:], jnp.float32)
        faces[s] = jnp.zeros(faces.shape[1:], jnp.float32)

    @pl.when(jnp.logical_not(has_before))
    def _():
        ghosts[0:n_new] = jnp.zeros((n_new, *ghosts.shape[1:]), jnp.float32)

    @pl.when(jnp.logical_not(has_after))
    def _():
        ghosts[2 * n_new :] = jnp.zeros((n_new, *ghosts.shape[1:]), jnp.float32)

    wide = 4 * edge
    l_row = iota((rows, 2 * rows), 0)
    l_col = iota((rows, 2 * rows), 1)
    l_col = jnp.where(l_col >= rows, l_col - rows, l_col)
    same_field = lax.div(l_row, edge) == lax.div(l_col, edge)
    for r in (1, 2):
        gap[r - 1] = (
            (lax.div(row, edge) - r * lax.div(col, edge)) * wide
            + lax.rem(row, edge)
            - r * lax.rem(col, edge)
        )
        near_x[r - 1] = jnp.where(
            same_field, lax.rem(l_col, edge) - r * lax.rem(l_row, edge), wide
        )

    for table in tables:
        table.wait()
    keys, ratios = [], []
    for p in range(n_pairs):
        target = pair_dest[p]
        owner = (lax.div(target, size_z) * size_y + iy) * size_z + lax.rem(target, size_z)
        keys.append(target * n_new + pair_slot[p])
        ratios.append(new_ratio[owner * n_new + pair_slot[p]])

    parts[n_pairs] = jnp.zeros(parts.shape[1:], jnp.float32)
    old_copy.wait()

    old_acc = [jnp.zeros((8, face), jnp.float32) for _ in range(fields)]
    for o in range(n_old):
        for f in range(fields):
            for h in range(edge // 8):
                old_acc[f] = old_acc[f] + old[o, f, h * 8 : (h + 1) * 8, :]

    new_acc = [jnp.zeros((8, face), jnp.float32) for _ in range(fields)]
    for p in range(n_pairs):
        ratio = ratios[p]
        coarse = ratio == 2
        kind = coarse.astype(jnp.int32)
        tx, ty, tz = pair_shift[0, p], pair_shift[1, p], pair_shift[2, p]
        scale = jnp.where(coarse, jnp.float32(0.125), jnp.float32(1.0))
        cube = jnp.where(coarse, jnp.float32(8.0), jnp.float32(1.0))
        inside = jnp.where(coarse, -2, -1)
        both_inside = jnp.where(coarse, -2 - wide, -1)
        block = old[pair_old[p]].reshape(rows, face)
        lx = ((near_x[kind] - tx) & inside) == 0
        lx = jnp.where(lx, 1.0, 0.0).astype(jnp.bfloat16)
        high, low = split_two(block)
        mixed = dot(lx, jnp.concatenate([high, low], axis=0))
        weight = ((gap[kind] - (ty * wide + tz)) & both_inside) == 0
        weight = jnp.where(weight, scale, jnp.float32(0.0)).astype(jnp.bfloat16)
        out = dot(jnp.concatenate(split_two(mixed), axis=0), weight)
        out = out[:rows] + out[rows:]
        for f in range(fields):
            for c in range(2):
                piece = out[f * edge + c * half : f * edge + (c + 1) * half]
                parts[p, c, f] = piece
                new_acc[f] = new_acc[f] + cube * piece

    pl.when(turn_after)(greet)

    def owner_sum(dst, x, s, core_of):
        target = chip_at(x) * 2 + core_of
        wanted = target * n_new + s
        first = jnp.int32(n_pairs)
        second = jnp.int32(n_pairs)
        for p in reversed(range(n_pairs)):
            hit = keys[p] == wanted
            second = jnp.where(hit, first, second)
            first = jnp.where(hit, jnp.int32(p), first)
        dst[x, :, s] = parts[first] + parts[second]

    orders, steps = plan_of(bits, n_new)

    def d2d_key(x, s):
        return (x, s) if x == chips - 1 else (x, None)

    d2d_order = []
    for _, _, x, s in steps:
        for t in range(n_new) if s is None else [s]:
            if d2d_key(x, t) not in d2d_order:
                d2d_order.append(d2d_key(x, t))
    d2d_order.append((0, None))

    def to_partner(key):
        x, s = key
        at = (x, slice(None), s) if s is not None else (x,)
        return pltpu.make_async_remote_copy(
            src_ref=theirs.at[at],
            dst_ref=partner_in.at[at],
            send_sem=d2d_send,
            recv_sem=d2d_recv.at[d2d_order.index(key)],
            device_id=partner,
            device_id_type=MESH,
        )

    def send_theirs(keys):
        for x, s in keys:
            for t in range(n_new) if s is None else [s]:
                owner_sum(theirs, x, t, 1 - core)
            to_partner((x, s)).start()

    send_theirs(d2d_order[:n_new])

    m_row = iota((16, 128), 0)
    m_col = iota((16, 128), 1)
    zero_rows = jnp.zeros((8 - fields, 128), jnp.float32)

    def lines(accs):
        out = [
            jnp.sum(a[:, :128] + a[:, 128:], axis=0, keepdims=True) for a in accs
        ]
        return out + [zero_rows]

    sums = jnp.concatenate(lines(old_acc) + lines(new_acc), axis=0)
    sums = jnp.sum(sums, axis=1, keepdims=True)
    sums = jnp.where(m_row == m_col, jnp.broadcast_to(sums, (16, 128)), 0.0)
    mass_own[0] = jnp.sum(sums, axis=0, keepdims=True)

    def mass_copy(k):
        return pltpu.make_async_remote_copy(
            src_ref=mass_own.at[k],
            dst_ref=mass_in.at[k],
            send_sem=mass_send.at[k],
            recv_sem=mass_recv.at[k],
            device_id=near_chip(k - 1) if k else partner,
            device_id_type=MESH,
        )

    def mass_join(k):
        mass_copy(k).wait_recv()
        mass_own[k + 1] = mass_own[k] + mass_in[k]

    mass_copy(0).start()

    send_theirs(d2d_order[n_new:])

    for x, s in d2d_order:
        for t in range(n_new) if s is None else [s]:
            owner_sum(mine, x, t, core)

    landed, joined = set(), set()

    def prepare(x, s):
        key = d2d_key(x, s)
        if key not in landed:
            landed.add(key)
            to_partner(key).wait_recv()
        if (x, s) not in joined:
            joined.add((x, s))
            mine[x, :, s] = mine[x, :, s] + partner_in[x, :, s]

    def to_chip(step):
        j, c, x, s = step
        here = (x, c) if s is None else (x, c, s)
        there = (x - 1, c) if s is None else (x - 1, c, s)
        return pltpu.make_async_remote_copy(
            src_ref=mine.at[here],
            dst_ref=chip_in.at[there],
            send_sem=chip_send,
            recv_sem=chip_recv.at[steps.index(step)],
            device_id=at_rank(chip_at(1 << orders[c][j]) * 2 + core),
            device_id_type=MESH,
        )

    waited = set()

    def take(c, x, s, j):
        total = mine[x, c, s]
        for b in orders[c][:j]:
            y = x | (1 << b)
            step = next(t for t in steps if t[1:3] == (c, y) and t[3] in (None, s))
            if step not in waited:
                waited.add(step)
                to_chip(step).wait_recv()
            total = total + chip_in[y - 1, c, s]
        return total

    leads = (core == 0) == (2 * iy < size_y)
    if LEAD_MODE == 1:
        leads = (core == 0) == (iy < size_y - 1)
    if LEAD_MODE == 2:
        leads = core == 0
    prepare(steps[0][2], 0)

    met = set()

    def meet(b):
        if b not in met:
            met.add(b)

            @pl.when(bit(b) == 0)
            def _():
                pl.semaphore_wait(near.at[b], 1)

    meet(0)

    def mass_first():
        mass_join(0)
        mass_copy(1).start()

    def all_of(ref, send_sem, recv_sem):
        return pltpu.make_async_remote_copy(
            src_ref=ref,
            dst_ref=ref,
            send_sem=send_sem,
            recv_sem=recv_sem,
            device_id=partner,
            device_id_type=MESH,
        )

    every_line = all_of(mass_line.at[1:], line_send, line_recv)
    beyond = size_y - 1 - iy + up.astype(jnp.int32) + turn_before.astype(jnp.int32)

    def to_line():
        for k in range(2, bits + 1):
            mass_join(k)
            if k < bits:
                meet(k)
                mass_copy(k + 1).start()
        mass_line[0] = mass_own[bits + 1]

        @pl.when(beyond > 0)
        def _():
            pl.semaphore_wait(far_ready, beyond)

        for k in range(1, size_y):
            pltpu.make_async_remote_copy(
                src_ref=mass_line.at[0],
                dst_ref=mass_line.at[k],
                send_sem=line_send,
                recv_sem=line_recv,
                device_id=(ix, lax.rem(iy + k, size_y), iz),
                device_id_type=MESH,
            ).start()

    late = [step for step in steps if step[0] == 0 and step[3] is None]
    first = [step for step in steps if step[0] == 0 and step[3] is not None]

    meet(orders[1][0])

    @pl.when(jnp.logical_not(leads))
    def _():
        mass_first()
        pl.semaphore_wait(turn, 1)

    for n, step in enumerate(first):
        if n == 2:
            pl.when(leads)(mass_first)
        prepare(step[2], step[3])
        to_chip(step).start()

    def pass_turn(at):
        if at not in (TURN_AT, TURN_LAST):
            return
        mine_now = leads
        if TURN_AT != TURN_LAST:
            mine_now = leads & (last_y if at == TURN_LAST else jnp.logical_not(last_y))

        @pl.when(mine_now)
        def _():
            signal(turn, partner)

    pass_turn(0)

    for step in late:
        for t in range(n_new):
            prepare(step[2], t)

    pass_turn(1)

    if EARLY_X1:

        @pl.when(leads)
        def _():
            for step in late:
                to_chip(step).start()

    mass_join(1)
    if bits > 1:
        meet(1)
        mass_copy(2).start()

    if not EARLY_X1:

        @pl.when(leads)
        def _():
            for step in late:
                to_chip(step).start()

    pass_turn(2)

    for step in steps:
        j, c, x, s = step
        if not j:
            continue
        meet(orders[c][j])
        for t in range(n_new) if s is None else [s]:
            prepare(x, t)
            mine[x, c, t] = take(c, x, t, j)
        if late:

            @pl.when(jnp.logical_not(leads))
            def _():
                for other in late:
                    to_chip(other).start()

            late = []
        to_chip(step).start()

    for s in range(n_new):
        prepare(0, s)

    to_line()

    tall = faces.shape[1]
    lane = iota((half, half * edge), 1)
    place = lax.div(lane, edge) == iota((half, half * edge), 0)
    along = lax.rem(lane, edge)
    spot_z = lax.rem(lane, half) * edge
    lower = along < half
    which = lax.rem(iota((tall, face), 0), 6)

    def pick(tile, spot):
        return jnp.take_along_axis(tile, spot, axis=1, mode="promise_in_bounds")

    def layers(block):
        left, right = block[:, : half * edge], block[:, half * edge :]
        found = [pick(left, along), pick(right, along + (half - 1) * edge)]
        for spot in (spot_z, spot_z + edge - 1):
            found.append(jnp.where(lower, pick(left, spot), pick(right, spot)))
        return [
            jnp.sum(jnp.where(place, one, 0.0), axis=0, keepdims=True) for one in found
        ]

    def face_copy(way, s):
        from_at, to_at = pl.ds(n_new, n_new), pl.ds(0 if way else 2 * n_new, n_new)
        if s is not None:
            from_at, to_at = n_new + s, s if way else 2 * n_new + s
        return pltpu.make_async_remote_copy(
            src_ref=ghosts.at[from_at],
            dst_ref=ghosts.at[to_at],
            send_sem=face_send.at[way],
            recv_sem=face_recv.at[way],
            device_id=at_linear(linear + 1 if way else linear - 1),
            device_id_type=MESH,
        )


    for s in range(n_new):
        for c in range(2):
            total = take(c, 0, s, bits)
            for f in range(fields):
                new_out[s, f, c * half : (c + 1) * half, :] = total[f]
        rows_of = []
        for f in range(fields):
            ends = [new_out[s, f, 0:1, :], new_out[s, f, edge - 1 : edge, :]]
            parts_of = [
                layers(new_out[s, f, c * half : (c + 1) * half, :]) for c in range(2)
            ]
            sides = [jnp.concatenate(pair, axis=1) for pair in zip(*parts_of)]
            rows_of.append(ends + sides)
            for e in range(6):
                at = 6 * f + e
                ghosts[n_new + s, at : at + 1, :] = rows_of[f][e ^ 1]

        @pl.when(has_after)
        def _(s=s):
            face_copy(1, s).start()

        @pl.when(has_before)
        def _(s=s):
            face_copy(0, s).start()

        for f in range(fields):
            for e in range(6):
                at = 6 * f + e
                faces[s, at : at + 1, :] = rows_of[f][e]

    every_line.wait_recv()
    total = jnp.zeros(mass_line.shape[1:], jnp.float32)
    for a in range(size_y):
        total = total + mass_line[lax.rem(iy - a + size_y, size_y)]
    total = total / float(n_old * devices * edge * face)
    for a in range(2):
        mass_out[a : a + 1, :] = total[:, 8 * a : 8 * a + fields]

    all_of(theirs, d2d_send, d2d_recv.at[0]).wait_send()
    all_of(chip_in, chip_send, chip_recv.at[0]).wait_send()
    for k in range(bits + 1):
        mass_copy(k).wait_send()
    every_line.wait_send()

    @pl.when(has_before)
    def _():
        face_copy(1, None).wait_recv()
        face_copy(0, None).wait_send()

    @pl.when(has_after)
    def _():
        face_copy(0, None).wait_recv()
        face_copy(1, None).wait_send()

    for s in range(n_new):
        ghost = jnp.zeros((tall, face), jnp.float32)
        present = jnp.zeros((tall, face), jnp.int32)
        for e in range(6):
            side = side_ref[s, e]
            source = linear + side - 1
            here = (side < 3) & (source >= 0) & (source < devices)
            place = jnp.where(side < 3, side, 0) * n_new + patch_ref[s, e]
            ghost = jnp.where(which == e, ghosts[place], ghost)
            present = jnp.where(which == e, here.astype(jnp.int32), present)
        jump = jnp.where(present > 0, ghost - faces[s], 0.0)
        for f in range(fields):
            jump_out[s, f] = jump[6 * f : 6 * f + 6]


def write_out(*refs):
    sems = refs[-1]
    copies = [pltpu.make_async_copy(refs[i], refs[3 + i], sems.at[i]) for i in range(3)]
    for copy in copies:
        copy.start()
    for copy in copies:
        copy.wait()


def body(
    old_data, pair_old, pair_slot, pair_shift, pair_dest, new_ratio, neighbor_side, neighbor_patch
):
    n_old, fields, edge, face = old_data.shape
    n_pairs = pair_old.shape[0]
    n_new = neighbor_side.shape[0]
    size_x, size_y, size_z = (lax.axis_size(a) for a in AXES)
    chips = size_x * size_z // 2
    assert size_z % 2 == 0 and chips & (chips - 1) == 0
    half = edge // 2
    bits = chips.bit_length() - 1
    tall = -(-6 * fields // 8) * 8
    dims = (size_x, size_y, size_z, n_old, n_new, n_pairs, fields, edge)
    f32 = jnp.float32
    vmem = pl.BlockSpec(memory_space=pltpu.VMEM)
    tables = (pair_old, pair_slot, pair_shift.T, pair_dest.reshape(n_pairs))
    tables += (new_ratio, neighbor_side, neighbor_patch)
    dma = pltpu.SemaphoreType.DMA
    shapes = ((n_new, fields, edge, face), (n_new, fields, 6, face), (2, fields))
    results = pl.pallas_call(
        functools.partial(kernel, dims),
        out_shape=tuple(pltpu.VMEM(s, f32) for s in shapes),
        in_specs=[pl.BlockSpec(memory_space=pl.ANY)] * 8,
        out_specs=(vmem, vmem, vmem),
        scratch_shapes=[pltpu.SMEM(t.shape, jnp.int32) for t in tables]
        + [
            pltpu.VMEM((2, face, face), jnp.int32),
            pltpu.VMEM((2, fields * edge, 2 * fields * edge), jnp.int32),
            pltpu.VMEM((n_old, fields, edge, face), f32),
            pltpu.VMEM((n_pairs + 1, 2, fields, half, face), f32),
            pltpu.VMEM((chips, 2, n_new, fields, half, face), f32),
            pltpu.VMEM((chips, 2, n_new, fields, half, face), f32),
            pltpu.VMEM((chips, 2, n_new, fields, half, face), f32),
            pltpu.VMEM((chips - 1, 2, n_new, fields, half, face), f32),
            pltpu.VMEM((n_new, tall, face), f32),
            pltpu.VMEM((3 * n_new, tall, face), f32),
            pltpu.VMEM((bits + 2, 1, 128), f32),
            pltpu.VMEM((bits + 1, 1, 128), f32),
            pltpu.VMEM((size_y, 1, 128), f32),
            dma,
            dma((len(tables),)),
            pltpu.SemaphoreType.REGULAR,
            pltpu.SemaphoreType.REGULAR((bits,)),
            pltpu.SemaphoreType.REGULAR,
            dma,
            dma((n_new + chips - 1,)),
            dma,
            dma((len(plan_of(bits, n_new)[1]),)),
            dma((2,)),
            dma((2,)),
            dma((bits + 1,)),
            dma((bits + 1,)),
            dma,
            dma,
        ],
        compiler_params=pltpu.CompilerParams(collective_id=0, has_side_effects=True),
    )(old_data, *tables)
    return pl.pallas_call(
        write_out,
        out_shape=tuple(jax.ShapeDtypeStruct(s, f32) for s in shapes),
        in_specs=[vmem] * 3,
        out_specs=(pl.BlockSpec(memory_space=pl.ANY),) * 3,
        scratch_shapes=[dma((3,))],
    )(*(pltpu.with_memory_space_constraint(r, pltpu.VMEM) for r in results))


def solution(mesh):
    whole = P(AXES)
    return jax.shard_map(
        body,
        mesh=mesh,
        in_specs=(whole, whole, whole, whole, whole, P(), whole, whole),
        out_specs=(whole, whole, P()),
        check_vma=False,
    )
```

```python
import functools

import jax
import jax.numpy as jnp
from jax import lax
from jax.experimental import pallas as pl
from jax.experimental.pallas import tpu as pltpu
from jax.sharding import PartitionSpec as P

MESH = pl.DeviceIdType.MESH
AXES = ("gx", "gy", "gz")


def split_two(value):
    high = value.astype(jnp.bfloat16)
    low = (value - high.astype(jnp.float32)).astype(jnp.bfloat16)
    return high, low


def dot(a, b):
    return jnp.dot(a, b, preferred_element_type=jnp.float32)


def iota(shape, axis):
    return lax.broadcasted_iota(jnp.int32, shape, axis)


def plan_of(bits, n_new, fields):
    chips = 1 << bits
    orders = [list(range(bits)), list(reversed(range(bits)))]

    def sends(order, j):
        done = sum(1 << b for b in order[:j])
        xs = [x for x in range(chips) if (x >> order[j]) & 1 and not x & done]
        return sorted(xs, key=lambda x: -bin(x).count("1"))

    steps = []
    whole, cut = (0, fields), fields // 4 * 4
    pieces = [(0, cut), (cut, fields)] if 0 < cut < fields else [whole]
    for j in range(bits):
        for pair in zip(*(sends(order, j) for order in orders)):
            fine = j == bits - 1 or pair[0] == chips - 1
            for s in range(n_new) if fine else [None]:
                last = j == bits - 1 and s == n_new - 1
                for r in pieces if last else [whole]:
                    for c in range(2):
                        steps.append((j, c, pair[c], s, r))
    return orders, steps, [[whole]] * (n_new - 1) + [pieces]


def kernel(
    dims,
    old_hbm,
    pair_old_hbm,
    pair_slot_hbm,
    pair_shift_hbm,
    pair_dest_hbm,
    new_ratio_hbm,
    side_hbm,
    patch_hbm,
    new_out,
    jump_out,
    mass_out,
    pair_old,
    pair_slot,
    pair_shift,
    pair_dest,
    new_ratio,
    side_ref,
    patch_ref,
    gap,
    near_x,
    old,
    parts,
    mine,
    theirs,
    inbox,
    faces,
    ghosts,
    mass_own,
    mass_in,
    old_sem,
    table_sem,
    turn,
    near,
    far_ready,
    bulk_send,
    d2d_recv,
    chip_recv,
    face_send,
    face_recv,
    mass_send,
    mass_recv,
    line_recv,
):
    size_x, size_y, size_z, n_old, n_new, n_pairs, fields, edge = dims
    face = edge * edge
    rows = fields * edge
    half = edge // 2
    group = size_x * size_z
    chips = group // 2
    bits = chips.bit_length() - 1
    devices = group * size_y
    ix, iy, iz = (lax.axis_index(a) for a in AXES)
    rank = ix * size_z + iz
    core = lax.rem(rank, 2)
    chip = lax.div(rank, 2)
    linear = (ix * size_y + iy) * size_z + iz

    def at_rank(g):
        return (lax.div(g, size_z), iy, lax.rem(g, size_z))

    def at_linear(d):
        return (
            lax.div(d, size_y * size_z),
            lax.rem(lax.div(d, size_z), size_y),
            lax.rem(d, size_z),
        )

    def chip_at(x):
        other = chip
        for b in range(bits):
            if (x >> b) & 1:
                other = other + (1 - 2 * lax.rem(lax.div(chip, 1 << b), 2)) * (1 << b)
        return other

    has_before = linear > 0
    has_after = linear < devices - 1
    partner = at_rank(chip * 2 + 1 - core)
    last_z = iz == size_z - 1
    first_z = iz == 0
    last_y = iy == size_y - 1
    first_y = iy == 0

    def signal(sem, device):
        pl.semaphore_signal(sem, inc=1, device_id=device, device_id_type=MESH)

    old_copy = pltpu.make_async_copy(old_hbm, old, old_sem)
    old_copy.start()
    tables = (
        (pair_dest_hbm, pair_dest),
        (pair_slot_hbm, pair_slot),
        (new_ratio_hbm, new_ratio),
        (pair_old_hbm, pair_old),
        (pair_shift_hbm, pair_shift),
        (side_hbm, side_ref),
        (patch_hbm, patch_ref),
    )
    tables = [
        pltpu.make_async_copy(source, table, table_sem.at[i])
        for i, (source, table) in enumerate(tables)
    ]
    for table in tables:
        table.start()

    def bit(b):
        return lax.rem(lax.div(chip, 1 << b), 2)

    def near_chip(b):
        return at_rank(chip_at(1 << b) * 2 + core)

    end = last_z & last_y
    start = first_z & first_y
    up = (core == 1) & has_after & jnp.logical_not(end)
    down = (core == 0) & has_before & jnp.logical_not(start)
    turn_after = end & has_after
    turn_before = start & has_before

    barrier = pltpu.get_barrier_semaphore()
    signal(barrier, partner)
    for b in range(bits):

        @pl.when(bit(b) == 0)
        def _(b=b):
            signal(barrier, near_chip(b))

    @pl.loop(iy + 1, size_y)
    def _(y):
        signal(barrier, (ix, y, iz))

    @pl.when(up)
    def _():
        signal(barrier, at_linear(linear + 1))

    @pl.when(turn_before)
    def _():
        signal(barrier, at_linear(linear - 1))

    count = 1 + iy + down.astype(jnp.int32) + turn_after.astype(jnp.int32)
    for b in range(bits):
        count = count + bit(b)

    def greet():
        pl.semaphore_wait(barrier, count)
        for b in range(bits):

            @pl.when(bit(b) == 1)
            def _(b=b):
                signal(near.at[b], near_chip(b))

        @pl.loop(0, iy)
        def _(y):
            signal(far_ready, (ix, y, iz))

        @pl.when(down)
        def _():
            signal(far_ready, at_linear(linear - 1))

        @pl.when(turn_after)
        def _():
            signal(far_ready, at_linear(linear + 1))

    pl.when(jnp.logical_not(turn_after))(greet)

    col = iota((face, face), 1)
    row = iota((face, face), 0)
    for s in range(n_new):
        ghosts[n_new + s] = jnp.zeros(ghosts.shape[1:], jnp.float32)
        faces[s] = jnp.zeros(faces.shape[1:], jnp.float32)

    @pl.when(jnp.logical_not(has_before))
    def _():
        ghosts[0:n_new] = jnp.zeros((n_new, *ghosts.shape[1:]), jnp.float32)

    @pl.when(jnp.logical_not(has_after))
    def _():
        ghosts[2 * n_new :] = jnp.zeros((n_new, *ghosts.shape[1:]), jnp.float32)

    wide = 4 * edge
    l_row = iota((rows, 2 * rows), 0)
    l_col = iota((rows, 2 * rows), 1)
    l_col = jnp.where(l_col >= rows, l_col - rows, l_col)
    same_field = lax.div(l_row, edge) == lax.div(l_col, edge)
    for r in (1, 2):
        gap[r - 1] = (
            (lax.div(row, edge) - r * lax.div(col, edge)) * wide
            + lax.rem(row, edge)
            - r * lax.rem(col, edge)
        )
        near_x[r - 1] = jnp.where(
            same_field, lax.rem(l_col, edge) - r * lax.rem(l_row, edge), wide
        )

    for table in tables:
        table.wait()
    keys, ratios = [], []
    for p in range(n_pairs):
        target = pair_dest[p]
        owner = (lax.div(target, size_z) * size_y + iy) * size_z + lax.rem(target, size_z)
        keys.append(target * n_new + pair_slot[p])
        ratios.append(new_ratio[owner * n_new + pair_slot[p]])

    parts[n_pairs] = jnp.zeros(parts.shape[1:], jnp.float32)
    old_copy.wait()

    new_acc = [jnp.zeros((8, face), jnp.float32) for _ in range(fields)]
    for p in range(n_pairs):
        ratio = ratios[p]
        coarse = ratio == 2
        kind = coarse.astype(jnp.int32)
        tx, ty, tz = pair_shift[0, p], pair_shift[1, p], pair_shift[2, p]
        scale = jnp.where(coarse, jnp.float32(0.125), jnp.float32(1.0))
        cube = jnp.where(coarse, jnp.float32(8.0), jnp.float32(1.0))
        inside = jnp.where(coarse, -2, -1)
        both_inside = jnp.where(coarse, -2 - wide, -1)
        block = old[pair_old[p]].reshape(rows, face)
        lx = ((near_x[kind] - tx) & inside) == 0
        lx = jnp.where(lx, 1.0, 0.0).astype(jnp.bfloat16)
        high, low = split_two(block)
        mixed = dot(lx, jnp.concatenate([high, low], axis=0))
        weight = ((gap[kind] - (ty * wide + tz)) & both_inside) == 0
        weight = jnp.where(weight, scale, jnp.float32(0.0)).astype(jnp.bfloat16)
        out = dot(jnp.concatenate(split_two(mixed), axis=0), weight)
        out = out[:rows] + out[rows:]
        for f in range(fields):
            for c in range(2):
                piece = out[f * edge + c * half : f * edge + (c + 1) * half]
                parts[p, c, f] = piece
                new_acc[f] = new_acc[f] + cube * piece

    pl.when(turn_after)(greet)

    def owner_sum(dst, x, s, core_of):
        target = chip_at(x) * 2 + core_of
        wanted = target * n_new + s
        first = jnp.int32(n_pairs)
        second = jnp.int32(n_pairs)
        for p in reversed(range(n_pairs)):
            hit = keys[p] == wanted
            second = jnp.where(hit, first, second)
            first = jnp.where(hit, jnp.int32(p), first)
        dst[x, :, s] = parts[first] + parts[second]

    orders, steps, pieces = plan_of(bits, n_new, fields)

    def d2d_key(x, s):
        return (x, s) if x == chips - 1 else (x, None)

    d2d_order = []
    for _, _, x, s, _ in steps:
        for t in range(n_new) if s is None else [s]:
            if d2d_key(x, t) not in d2d_order:
                d2d_order.append(d2d_key(x, t))
    d2d_order.append((0, None))

    def to_partner(key):
        x, s = key
        at = (x, slice(None), s) if s is not None else (x,)
        return pltpu.make_async_remote_copy(
            src_ref=theirs.at[at],
            dst_ref=inbox.at[at],
            send_sem=bulk_send,
            recv_sem=d2d_recv.at[d2d_order.index(key)],
            device_id=partner,
            device_id_type=MESH,
        )

    def send_theirs(keys):
        for x, s in keys:
            for t in range(n_new) if s is None else [s]:
                owner_sum(theirs, x, t, 1 - core)
            to_partner((x, s)).start()

    send_theirs(d2d_order[:n_new])

    old_acc = [jnp.zeros((8, face), jnp.float32) for _ in range(fields)]
    for o in range(n_old):
        for f in range(fields):
            for h in range(edge // 8):
                old_acc[f] = old_acc[f] + old[o, f, h * 8 : (h + 1) * 8, :]

    m_row = iota((16, 128), 0)
    m_col = iota((16, 128), 1)
    zero_rows = jnp.zeros((8 - fields, 128), jnp.float32)

    def lines(accs):
        out = [
            jnp.sum(a[:, :128] + a[:, 128:], axis=0, keepdims=True) for a in accs
        ]
        return out + [zero_rows]

    sums = jnp.concatenate(lines(old_acc) + lines(new_acc), axis=0)
    sums = jnp.sum(sums, axis=1, keepdims=True)
    sums = jnp.where(m_row == m_col, jnp.broadcast_to(sums, (16, 128)), 0.0)
    mass_own[0] = jnp.sum(sums, axis=0, keepdims=True)

    def mass_copy(k):
        return pltpu.make_async_remote_copy(
            src_ref=mass_own.at[k],
            dst_ref=mass_in.at[k],
            send_sem=mass_send,
            recv_sem=mass_recv.at[k],
            device_id=near_chip(k - 1) if k else partner,
            device_id_type=MESH,
        )

    def mass_join(k):
        mass_copy(k).wait_recv()
        mass_own[k + 1] = mass_own[k] + mass_in[k]

    mass_copy(0).start()

    send_theirs(d2d_order[n_new:])

    for x, s in d2d_order:
        for t in range(n_new) if s is None else [s]:
            owner_sum(mine, x, t, core)

    landed, joined = set(), set()

    def prepare(x, s):
        key = d2d_key(x, s)
        if key not in landed:
            landed.add(key)
            to_partner(key).wait_recv()
        if (x, s) not in joined:
            joined.add((x, s))
            mine[x, :, s] = mine[x, :, s] + inbox[x, :, s]

    def to_chip(step):
        j, c, x, s, r = step
        cut = () if s is None else (s,) if r == (0, fields) else (s, slice(*r))
        here = (x, c) + cut
        there = (chips + x - 1, c) + cut
        return pltpu.make_async_remote_copy(
            src_ref=mine.at[here],
            dst_ref=inbox.at[there],
            send_sem=bulk_send,
            recv_sem=chip_recv.at[steps.index(step)],
            device_id=at_rank(chip_at(1 << orders[c][j]) * 2 + core),
            device_id_type=MESH,
        )

    waited = set()

    def take(c, x, s, j, r):
        total = mine[x, c, s, r[0] : r[1]]
        for b in orders[c][:j]:
            y = x | (1 << b)
            step = next(
                t
                for t in steps
                if t[1:3] == (c, y) and t[3] in (None, s) and t[4] in ((0, fields), r)
            )
            if step not in waited:
                waited.add(step)
                to_chip(step).wait_recv()
            total = total + inbox[chips + y - 1, c, s, r[0] : r[1]]
        return total

    leads = (core == 0) == (iy < size_y - 1)
    prepare(steps[0][2], 0)

    met = set()

    def meet(b):
        if b not in met:
            met.add(b)

            @pl.when(bit(b) == 0)
            def _():
                pl.semaphore_wait(near.at[b], 1)

    meet(0)

    def mass_first():
        mass_join(0)
        mass_copy(1).start()

    def all_of(ref, send_sem, recv_sem):
        return pltpu.make_async_remote_copy(
            src_ref=ref,
            dst_ref=ref,
            send_sem=send_sem,
            recv_sem=recv_sem,
            device_id=partner,
            device_id_type=MESH,
        )

    first_line = bits + 1
    every_line = all_of(mass_in.at[first_line + 1 :], mass_send, line_recv)
    beyond = size_y - 1 - iy + up.astype(jnp.int32) + turn_before.astype(jnp.int32)

    def to_line():
        for k in range(2, bits + 1):
            mass_join(k)
            if k < bits:
                meet(k)
                mass_copy(k + 1).start()
        mass_in[first_line] = mass_own[bits + 1]

        @pl.when(beyond > 0)
        def _():
            pl.semaphore_wait(far_ready, beyond)

        for k in range(1, size_y):
            pltpu.make_async_remote_copy(
                src_ref=mass_in.at[first_line],
                dst_ref=mass_in.at[first_line + k],
                send_sem=mass_send,
                recv_sem=line_recv,
                device_id=(ix, lax.rem(iy + k, size_y), iz),
                device_id_type=MESH,
            ).start()

    late = [step for step in steps if step[0] == 0 and step[3] is None]
    first = [step for step in steps if step[0] == 0 and step[3] is not None]

    meet(orders[1][0])

    @pl.when(jnp.logical_not(leads))
    def _():
        mass_first()
        pl.semaphore_wait(turn, 1)

    for n, step in enumerate(first):
        if n == 2:
            pl.when(leads)(mass_first)
        prepare(step[2], step[3])
        to_chip(step).start()

    def pass_turn(now):
        @pl.when(leads & now)
        def _():
            signal(turn, partner)

    pass_turn(last_y)

    for step in late:
        for t in range(n_new):
            prepare(step[2], t)

    @pl.when(leads & jnp.logical_not(last_y))
    def _():
        for step in late:
            to_chip(step).start()

    mass_join(1)
    if bits > 1:
        meet(1)
        mass_copy(2).start()

    @pl.when(leads & last_y)
    def _():
        for step in late:
            to_chip(step).start()

    pass_turn(jnp.logical_not(last_y))

    for step in steps:
        j, c, x, s, r = step
        if not j:
            continue
        meet(orders[c][j])
        for t in range(n_new) if s is None else [s]:
            prepare(x, t)
            mine[x, c, t, r[0] : r[1]] = take(c, x, t, j, r)
        if late:

            @pl.when(jnp.logical_not(leads))
            def _():
                for other in late:
                    to_chip(other).start()

            late = []
        to_chip(step).start()

    for s in range(n_new):
        prepare(0, s)

    to_line()

    tall = faces.shape[1]
    lane = iota((half, half * edge), 1)
    place = lax.div(lane, edge) == iota((half, half * edge), 0)
    along = lax.rem(lane, edge)
    spot_z = lax.rem(lane, half) * edge
    lower = along < half
    which = lax.rem(iota((tall, face), 0), 6)

    def pick(tile, spot):
        return jnp.take_along_axis(tile, spot, axis=1, mode="promise_in_bounds")

    def layers(block):
        left, right = block[:, : half * edge], block[:, half * edge :]
        found = [pick(left, along), pick(right, along + (half - 1) * edge)]
        for spot in (spot_z, spot_z + edge - 1):
            found.append(jnp.where(lower, pick(left, spot), pick(right, spot)))
        return [
            jnp.sum(jnp.where(place, one, 0.0), axis=0, keepdims=True) for one in found
        ]

    def face_copy(way, s, r=None):
        rows_at = () if r is None else (pl.ds(6 * r[0], (6 * r[1] + 7) // 8 * 8 - 6 * r[0]),)
        from_at, to_at = pl.ds(n_new, n_new), pl.ds(0 if way else 2 * n_new, n_new)
        if s is not None:
            from_at, to_at = n_new + s, s if way else 2 * n_new + s
        return pltpu.make_async_remote_copy(
            src_ref=ghosts.at[(from_at,) + rows_at],
            dst_ref=ghosts.at[(to_at,) + rows_at],
            send_sem=face_send.at[way],
            recv_sem=face_recv.at[way],
            device_id=at_linear(linear + 1 if way else linear - 1),
            device_id_type=MESH,
        )

    for s in range(n_new):
        for r in pieces[s]:
            for c in range(2):
                total = take(c, 0, s, bits, r)
                for f in range(*r):
                    new_out[s, f, c * half : (c + 1) * half, :] = total[f - r[0]]
            rows_of = {}
            for f in range(*r):
                ends = [new_out[s, f, 0:1, :], new_out[s, f, edge - 1 : edge, :]]
                parts_of = [
                    layers(new_out[s, f, c * half : (c + 1) * half, :]) for c in range(2)
                ]
                sides = [jnp.concatenate(pair, axis=1) for pair in zip(*parts_of)]
                rows_of[f] = ends + sides
                for e in range(6):
                    at = 6 * f + e
                    ghosts[n_new + s, at : at + 1, :] = rows_of[f][e ^ 1]

            @pl.when(has_after)
            def _(s=s, r=r):
                face_copy(1, s, r).start()

            @pl.when(has_before)
            def _(s=s, r=r):
                face_copy(0, s, r).start()

            for f in range(*r):
                for e in range(6):
                    at = 6 * f + e
                    faces[s, at : at + 1, :] = rows_of[f][e]

    every_line.wait_recv()
    total = jnp.zeros(mass_in.shape[1:], jnp.float32)
    for a in range(size_y):
        total = total + mass_in[first_line + lax.rem(iy - a + size_y, size_y)]
    total = total / float(n_old * devices * edge * face)
    for a in range(2):
        mass_out[a : a + 1, :] = total[:, 8 * a : 8 * a + fields]

    all_of(inbox, bulk_send, chip_recv.at[0]).wait_send()
    all_of(mass_in.at[: bits + size_y], mass_send, line_recv).wait_send()

    @pl.when(has_before)
    def _():
        face_copy(1, None).wait_recv()
        face_copy(0, None).wait_send()

    @pl.when(has_after)
    def _():
        face_copy(0, None).wait_recv()
        face_copy(1, None).wait_send()

    for s in range(n_new):
        ghost = jnp.zeros((tall, face), jnp.float32)
        present = jnp.zeros((tall, face), jnp.int32)
        for e in range(6):
            side = side_ref[s, e]
            source = linear + side - 1
            here = (side < 3) & (source >= 0) & (source < devices)
            place = jnp.where(side < 3, side, 0) * n_new + patch_ref[s, e]
            ghost = jnp.where(which == e, ghosts[place], ghost)
            present = jnp.where(which == e, here.astype(jnp.int32), present)
        jump = jnp.where(present > 0, ghost - faces[s], 0.0)
        for f in range(fields):
            jump_out[s, f] = jump[6 * f : 6 * f + 6]


def write_out(*refs):
    sems = refs[-1]
    copies = [pltpu.make_async_copy(refs[i], refs[3 + i], sems.at[i]) for i in range(3)]
    for copy in copies:
        copy.start()
    for copy in copies:
        copy.wait()


def body(
    old_data, pair_old, pair_slot, pair_shift, pair_dest, new_ratio, neighbor_side, neighbor_patch
):
    n_old, fields, edge, face = old_data.shape
    n_pairs = pair_old.shape[0]
    n_new = neighbor_side.shape[0]
    size_x, size_y, size_z = (lax.axis_size(a) for a in AXES)
    chips = size_x * size_z // 2
    assert size_z % 2 == 0 and chips & (chips - 1) == 0
    half = edge // 2
    bits = chips.bit_length() - 1
    tall = -(-6 * fields // 8) * 8
    dims = (size_x, size_y, size_z, n_old, n_new, n_pairs, fields, edge)
    f32 = jnp.float32
    vmem = pl.BlockSpec(memory_space=pltpu.VMEM)
    tables = (pair_old, pair_slot, pair_shift.T, pair_dest.reshape(n_pairs))
    tables += (new_ratio, neighbor_side, neighbor_patch)
    dma = pltpu.SemaphoreType.DMA
    shapes = ((n_new, fields, edge, face), (n_new, fields, 6, face), (2, fields))
    results = pl.pallas_call(
        functools.partial(kernel, dims),
        out_shape=tuple(pltpu.VMEM(s, f32) for s in shapes),
        in_specs=[pl.BlockSpec(memory_space=pl.ANY)] * 8,
        out_specs=(vmem, vmem, vmem),
        scratch_shapes=[pltpu.SMEM(t.shape, jnp.int32) for t in tables]
        + [
            pltpu.VMEM((2, face, face), jnp.int32),
            pltpu.VMEM((2, fields * edge, 2 * fields * edge), jnp.int32),
            pltpu.VMEM((n_old, fields, edge, face), f32),
            pltpu.VMEM((n_pairs + 1, 2, fields, half, face), f32),
            pltpu.VMEM((chips, 2, n_new, fields, half, face), f32),
            pltpu.VMEM((chips, 2, n_new, fields, half, face), f32),
            pltpu.VMEM((2 * chips - 1, 2, n_new, fields, half, face), f32),
            pltpu.VMEM((n_new, tall, face), f32),
            pltpu.VMEM((3 * n_new, tall, face), f32),
            pltpu.VMEM((bits + 2, 1, 128), f32),
            pltpu.VMEM((bits + 1 + size_y, 1, 128), f32),
            dma,
            dma((len(tables),)),
            pltpu.SemaphoreType.REGULAR,
            pltpu.SemaphoreType.REGULAR((bits,)),
            pltpu.SemaphoreType.REGULAR,
            dma,
            dma((n_new + chips - 1,)),
            dma((len(plan_of(bits, n_new, fields)[1]),)),
            dma((2,)),
            dma((2,)),
            dma,
            dma((bits + 1,)),
            dma,
        ],
        compiler_params=pltpu.CompilerParams(collective_id=0, has_side_effects=True),
    )(old_data, *tables)
    return pl.pallas_call(
        write_out,
        out_shape=tuple(jax.ShapeDtypeStruct(s, f32) for s in shapes),
        in_specs=[vmem] * 3,
        out_specs=(pl.BlockSpec(memory_space=pl.ANY),) * 3,
        scratch_shapes=[dma((3,))],
    )(*(pltpu.with_memory_space_constraint(r, pltpu.VMEM) for r in results))


def solution(mesh):
    whole = P(AXES)
    return jax.shard_map(
        body,
        mesh=mesh,
        in_specs=(whole, whole, whole, whole, whole, P(), whole, whole),
        out_specs=(whole, whole, P()),
        check_vma=False,
    )
```

```python
import functools

import jax
import jax.numpy as jnp
from jax import lax
from jax.experimental import pallas as pl
from jax.experimental.pallas import tpu as pltpu
from jax.sharding import PartitionSpec as P

MESH = pl.DeviceIdType.MESH
AXES = ("gx", "gy", "gz")


def split_two(value):
    high = value.astype(jnp.bfloat16)
    low = (value - high.astype(jnp.float32)).astype(jnp.bfloat16)
    return high, low


def dot(a, b):
    return jnp.dot(a, b, preferred_element_type=jnp.float32)


def iota(shape, axis):
    return lax.broadcasted_iota(jnp.int32, shape, axis)


def plan_of(bits, n_new, fields):
    chips = 1 << bits
    orders = [list(range(bits)), list(reversed(range(bits)))]

    def sends(order, j):
        done = sum(1 << b for b in order[:j])
        xs = [x for x in range(chips) if (x >> order[j]) & 1 and not x & done]
        return sorted(xs, key=lambda x: -bin(x).count("1"))

    steps = []
    whole, cut = (0, fields), fields // 4 * 4
    pieces = [(0, cut), (cut, fields)] if 0 < cut < fields else [whole]
    for j in range(bits):
        for pair in zip(*(sends(order, j) for order in orders)):
            fine = j == bits - 1 or pair[0] == chips - 1
            for s in range(n_new) if fine else [None]:
                last = j == bits - 1 and s == n_new - 1
                for r in pieces if last else [whole]:
                    for c in range(2):
                        steps.append((j, c, pair[c], s, r))
    return orders, steps, [[whole]] * (n_new - 1) + [pieces]


def kernel(
    dims,
    old_hbm,
    pair_old_hbm,
    pair_slot_hbm,
    pair_shift_hbm,
    pair_dest_hbm,
    new_ratio_hbm,
    side_hbm,
    patch_hbm,
    new_out,
    jump_out,
    mass_out,
    pair_old,
    pair_slot,
    pair_shift,
    pair_dest,
    new_ratio,
    side_ref,
    patch_ref,
    gap,
    near_x,
    old,
    parts,
    mine,
    theirs,
    inbox,
    faces,
    ghosts,
    mass_own,
    mass_in,
    old_sem,
    table_sem,
    turn,
    near,
    far_ready,
    bulk_send,
    d2d_recv,
    chip_recv,
    face_send,
    face_recv,
    mass_send,
    mass_recv,
    line_recv,
):
    size_x, size_y, size_z, n_old, n_new, n_pairs, fields, edge = dims
    face = edge * edge
    rows = fields * edge
    half = edge // 2
    group = size_x * size_z
    chips = group // 2
    bits = chips.bit_length() - 1
    devices = group * size_y
    ix, iy, iz = (lax.axis_index(a) for a in AXES)
    rank = ix * size_z + iz
    core = lax.rem(rank, 2)
    chip = lax.div(rank, 2)
    linear = (ix * size_y + iy) * size_z + iz

    def at_rank(g):
        return (lax.div(g, size_z), iy, lax.rem(g, size_z))

    def at_linear(d):
        return (
            lax.div(d, size_y * size_z),
            lax.rem(lax.div(d, size_z), size_y),
            lax.rem(d, size_z),
        )

    def chip_at(x):
        other = chip
        for b in range(bits):
            if (x >> b) & 1:
                other = other + (1 - 2 * lax.rem(lax.div(chip, 1 << b), 2)) * (1 << b)
        return other

    has_before = linear > 0
    has_after = linear < devices - 1
    partner = at_rank(chip * 2 + 1 - core)
    last_z = iz == size_z - 1
    first_z = iz == 0
    last_y = iy == size_y - 1
    first_y = iy == 0

    def signal(sem, device):
        pl.semaphore_signal(sem, inc=1, device_id=device, device_id_type=MESH)

    old_copy = pltpu.make_async_copy(old_hbm, old, old_sem)
    old_copy.start()
    tables = (
        (pair_dest_hbm, pair_dest),
        (pair_slot_hbm, pair_slot),
        (new_ratio_hbm, new_ratio),
        (pair_old_hbm, pair_old),
        (pair_shift_hbm, pair_shift),
        (side_hbm, side_ref),
        (patch_hbm, patch_ref),
    )
    tables = [
        pltpu.make_async_copy(source, table, table_sem.at[i])
        for i, (source, table) in enumerate(tables)
    ]
    for table in tables:
        table.start()

    def bit(b):
        return lax.rem(lax.div(chip, 1 << b), 2)

    def near_chip(b):
        return at_rank(chip_at(1 << b) * 2 + core)

    end = last_z & last_y
    start = first_z & first_y
    up = (core == 1) & has_after & jnp.logical_not(end)
    down = (core == 0) & has_before & jnp.logical_not(start)
    turn_after = end & has_after
    turn_before = start & has_before

    barrier = pltpu.get_barrier_semaphore()
    signal(barrier, partner)
    for b in range(bits):

        @pl.when(bit(b) == 0)
        def _(b=b):
            signal(barrier, near_chip(b))

    @pl.loop(iy + 1, size_y)
    def _(y):
        signal(barrier, (ix, y, iz))

    @pl.when(up)
    def _():
        signal(barrier, at_linear(linear + 1))

    @pl.when(turn_before)
    def _():
        signal(barrier, at_linear(linear - 1))

    count = 1 + iy + down.astype(jnp.int32) + turn_after.astype(jnp.int32)
    for b in range(bits):
        count = count + bit(b)

    def greet():
        pl.semaphore_wait(barrier, count)
        for b in range(bits):

            @pl.when(bit(b) == 1)
            def _(b=b):
                signal(near.at[b], near_chip(b))

        @pl.loop(0, iy)
        def _(y):
            signal(far_ready, (ix, y, iz))

        @pl.when(down)
        def _():
            signal(far_ready, at_linear(linear - 1))

        @pl.when(turn_after)
        def _():
            signal(far_ready, at_linear(linear + 1))

    pl.when(jnp.logical_not(turn_after))(greet)

    col = iota((face, face), 1)
    row = iota((face, face), 0)
    for s in range(n_new):
        ghosts[n_new + s] = jnp.zeros(ghosts.shape[1:], jnp.float32)
        faces[s] = jnp.zeros(faces.shape[1:], jnp.float32)

    @pl.when(jnp.logical_not(has_before))
    def _():
        ghosts[0:n_new] = jnp.zeros((n_new, *ghosts.shape[1:]), jnp.float32)

    @pl.when(jnp.logical_not(has_after))
    def _():
        ghosts[2 * n_new :] = jnp.zeros((n_new, *ghosts.shape[1:]), jnp.float32)

    wide = 4 * edge
    l_row = iota((rows, 2 * rows), 0)
    l_col = iota((rows, 2 * rows), 1)
    l_col = jnp.where(l_col >= rows, l_col - rows, l_col)
    same_field = lax.div(l_row, edge) == lax.div(l_col, edge)
    for r in (1, 2):
        gap[r - 1] = (
            (lax.div(row, edge) - r * lax.div(col, edge)) * wide
            + lax.rem(row, edge)
            - r * lax.rem(col, edge)
        )
        near_x[r - 1] = jnp.where(
            same_field, lax.rem(l_col, edge) - r * lax.rem(l_row, edge), wide
        )

    for table in tables:
        table.wait()
    keys, ratios = [], []
    for p in range(n_pairs):
        target = pair_dest[p]
        owner = (lax.div(target, size_z) * size_y + iy) * size_z + lax.rem(target, size_z)
        keys.append(target * n_new + pair_slot[p])
        ratios.append(new_ratio[owner * n_new + pair_slot[p]])

    parts[n_pairs] = jnp.zeros(parts.shape[1:], jnp.float32)
    old_copy.wait()

    new_acc = [jnp.zeros((8, face), jnp.float32) for _ in range(fields)]
    for p in range(n_pairs):
        ratio = ratios[p]
        coarse = ratio == 2
        kind = coarse.astype(jnp.int32)
        tx, ty, tz = pair_shift[0, p], pair_shift[1, p], pair_shift[2, p]
        scale = jnp.where(coarse, jnp.float32(0.125), jnp.float32(1.0))
        cube = jnp.where(coarse, jnp.float32(8.0), jnp.float32(1.0))
        inside = jnp.where(coarse, -2, -1)
        both_inside = jnp.where(coarse, -2 - wide, -1)
        block = old[pair_old[p]].reshape(rows, face)
        lx = ((near_x[kind] - tx) & inside) == 0
        lx = jnp.where(lx, 1.0, 0.0).astype(jnp.bfloat16)
        high, low = split_two(block)
        mixed = dot(lx, jnp.concatenate([high, low], axis=0))
        weight = ((gap[kind] - (ty * wide + tz)) & both_inside) == 0
        weight = jnp.where(weight, scale, jnp.float32(0.0)).astype(jnp.bfloat16)
        out = dot(jnp.concatenate(split_two(mixed), axis=0), weight)
        out = out[:rows] + out[rows:]
        for f in range(fields):
            for c in range(2):
                piece = out[f * edge + c * half : f * edge + (c + 1) * half]
                parts[p, c, f] = piece
                new_acc[f] = new_acc[f] + cube * piece

    pl.when(turn_after)(greet)

    def owner_sum(dst, x, s, core_of):
        target = chip_at(x) * 2 + core_of
        wanted = target * n_new + s
        first = jnp.int32(n_pairs)
        second = jnp.int32(n_pairs)
        for p in reversed(range(n_pairs)):
            hit = keys[p] == wanted
            second = jnp.where(hit, first, second)
            first = jnp.where(hit, jnp.int32(p), first)
        dst[x, :, s] = parts[first] + parts[second]

    orders, steps, pieces = plan_of(bits, n_new, fields)

    def d2d_key(x, s):
        return (x, s) if x == chips - 1 else (x, None)

    d2d_order = []
    for _, _, x, s, _ in steps:
        for t in range(n_new) if s is None else [s]:
            if d2d_key(x, t) not in d2d_order:
                d2d_order.append(d2d_key(x, t))
    d2d_order.append((0, None))

    def to_partner(key):
        x, s = key
        at = (x, slice(None), s) if s is not None else (x,)
        return pltpu.make_async_remote_copy(
            src_ref=theirs.at[at],
            dst_ref=inbox.at[at],
            send_sem=bulk_send,
            recv_sem=d2d_recv.at[d2d_order.index(key)],
            device_id=partner,
            device_id_type=MESH,
        )

    def send_theirs(keys):
        for x, s in keys:
            for t in range(n_new) if s is None else [s]:
                owner_sum(theirs, x, t, 1 - core)
            to_partner((x, s)).start()

    send_theirs(d2d_order[:n_new])

    old_acc = [jnp.zeros((8, face), jnp.float32) for _ in range(fields)]
    for o in range(n_old):
        for f in range(fields):
            for h in range(edge // 8):
                old_acc[f] = old_acc[f] + old[o, f, h * 8 : (h + 1) * 8, :]

    m_row = iota((16, 128), 0)
    m_col = iota((16, 128), 1)
    zero_rows = jnp.zeros((8 - fields, 128), jnp.float32)

    def lines(accs):
        out = [
            jnp.sum(a[:, :128] + a[:, 128:], axis=0, keepdims=True) for a in accs
        ]
        return out + [zero_rows]

    sums = jnp.concatenate(lines(old_acc) + lines(new_acc), axis=0)
    sums = jnp.sum(sums, axis=1, keepdims=True)
    sums = jnp.where(m_row == m_col, jnp.broadcast_to(sums, (16, 128)), 0.0)
    mass_own[0] = jnp.sum(sums, axis=0, keepdims=True)

    def mass_copy(k):
        return pltpu.make_async_remote_copy(
            src_ref=mass_own.at[k],
            dst_ref=mass_in.at[k],
            send_sem=mass_send,
            recv_sem=mass_recv.at[k],
            device_id=near_chip(k - 1) if k else partner,
            device_id_type=MESH,
        )

    def mass_join(k):
        mass_copy(k).wait_recv()
        mass_own[k + 1] = mass_own[k] + mass_in[k]

    mass_copy(0).start()

    send_theirs(d2d_order[n_new:])

    for x, s in d2d_order:
        for t in range(n_new) if s is None else [s]:
            owner_sum(mine, x, t, core)

    landed, joined = set(), set()

    def prepare(x, s):
        key = d2d_key(x, s)
        if key not in landed:
            landed.add(key)
            to_partner(key).wait_recv()
        if (x, s) not in joined:
            joined.add((x, s))
            mine[x, :, s] = mine[x, :, s] + inbox[x, :, s]

    def to_chip(step):
        j, c, x, s, r = step
        cut = () if s is None else (s,) if r == (0, fields) else (s, slice(*r))
        here = (x, c) + cut
        there = (chips + x - 1, c) + cut
        return pltpu.make_async_remote_copy(
            src_ref=mine.at[here],
            dst_ref=inbox.at[there],
            send_sem=bulk_send,
            recv_sem=chip_recv.at[steps.index(step)],
            device_id=at_rank(chip_at(1 << orders[c][j]) * 2 + core),
            device_id_type=MESH,
        )

    waited = set()

    def take(c, x, s, j, r):
        total = mine[x, c, s, r[0] : r[1]]
        for b in orders[c][:j]:
            y = x | (1 << b)
            step = next(
                t
                for t in steps
                if t[1:3] == (c, y) and t[3] in (None, s) and t[4] in ((0, fields), r)
            )
            if step not in waited:
                waited.add(step)
                to_chip(step).wait_recv()
            total = total + inbox[chips + y - 1, c, s, r[0] : r[1]]
        return total

    leads = (core == 0) == (iy < size_y - 1)
    prepare(steps[0][2], 0)

    met = set()

    def meet(b):
        if b not in met:
            met.add(b)

            @pl.when(bit(b) == 0)
            def _():
                pl.semaphore_wait(near.at[b], 1)

    meet(0)

    def mass_first():
        mass_join(0)
        mass_copy(1).start()

    def all_of(ref, send_sem, recv_sem):
        return pltpu.make_async_remote_copy(
            src_ref=ref,
            dst_ref=ref,
            send_sem=send_sem,
            recv_sem=recv_sem,
            device_id=partner,
            device_id_type=MESH,
        )

    first_line = bits + 1
    every_line = all_of(mass_in.at[first_line + 1 :], mass_send, line_recv)
    beyond = size_y - 1 - iy + up.astype(jnp.int32) + turn_before.astype(jnp.int32)

    def to_line():
        for k in range(2, bits + 1):
            mass_join(k)
            if k < bits:
                meet(k)
                mass_copy(k + 1).start()
        mass_in[first_line] = mass_own[bits + 1]

        @pl.when(beyond > 0)
        def _():
            pl.semaphore_wait(far_ready, beyond)

        for k in range(1, size_y):
            pltpu.make_async_remote_copy(
                src_ref=mass_in.at[first_line],
                dst_ref=mass_in.at[first_line + k],
                send_sem=mass_send,
                recv_sem=line_recv,
                device_id=(ix, lax.rem(iy + k, size_y), iz),
                device_id_type=MESH,
            ).start()

    late = [step for step in steps if step[0] == 0 and step[3] is None]
    first = [step for step in steps if step[0] == 0 and step[3] is not None]

    meet(orders[1][0])

    @pl.when(jnp.logical_not(leads))
    def _():
        mass_first()
        pl.semaphore_wait(turn, 1)

    for n, step in enumerate(first):
        if n == 2:
            pl.when(leads)(mass_first)
        prepare(step[2], step[3])
        to_chip(step).start()

    def pass_turn(now):
        @pl.when(leads & now)
        def _():
            signal(turn, partner)

    for step in late:
        for t in range(n_new):
            prepare(step[2], t)

    pass_turn(last_y)

    @pl.when(leads)
    def _():
        for step in late:
            to_chip(step).start()

    mass_join(1)
    if bits > 1:
        meet(1)
        mass_copy(2).start()

    pass_turn(jnp.logical_not(last_y))

    for step in steps:
        j, c, x, s, r = step
        if not j:
            continue
        meet(orders[c][j])
        for t in range(n_new) if s is None else [s]:
            prepare(x, t)
            mine[x, c, t, r[0] : r[1]] = take(c, x, t, j, r)
        if late:

            @pl.when(jnp.logical_not(leads))
            def _():
                for other in late:
                    to_chip(other).start()

            late = []
        to_chip(step).start()

    for s in range(n_new):
        prepare(0, s)

    to_line()

    tall = faces.shape[1]
    lane = iota((half, half * edge), 1)
    place = lax.div(lane, edge) == iota((half, half * edge), 0)
    along = lax.rem(lane, edge)
    spot_z = lax.rem(lane, half) * edge
    lower = along < half
    which = lax.rem(iota((tall, face), 0), 6)

    def pick(tile, spot):
        return jnp.take_along_axis(tile, spot, axis=1, mode="promise_in_bounds")

    def layers(block):
        left, right = block[:, : half * edge], block[:, half * edge :]
        found = [pick(left, along), pick(right, along + (half - 1) * edge)]
        for spot in (spot_z, spot_z + edge - 1):
            found.append(jnp.where(lower, pick(left, spot), pick(right, spot)))
        return [
            jnp.sum(jnp.where(place, one, 0.0), axis=0, keepdims=True) for one in found
        ]

    def face_copy(way, s, r=None):
        rows_at = () if r is None else (pl.ds(6 * r[0], (6 * r[1] + 7) // 8 * 8 - 6 * r[0]),)
        from_at, to_at = pl.ds(n_new, n_new), pl.ds(0 if way else 2 * n_new, n_new)
        if s is not None:
            from_at, to_at = n_new + s, s if way else 2 * n_new + s
        return pltpu.make_async_remote_copy(
            src_ref=ghosts.at[(from_at,) + rows_at],
            dst_ref=ghosts.at[(to_at,) + rows_at],
            send_sem=face_send.at[way],
            recv_sem=face_recv.at[way],
            device_id=at_linear(linear + 1 if way else linear - 1),
            device_id_type=MESH,
        )

    for s in range(n_new):
        for r in pieces[s]:
            for c in range(2):
                total = take(c, 0, s, bits, r)
                for f in range(*r):
                    new_out[s, f, c * half : (c + 1) * half, :] = total[f - r[0]]
            rows_of = {}
            for f in range(*r):
                ends = [new_out[s, f, 0:1, :], new_out[s, f, edge - 1 : edge, :]]
                parts_of = [
                    layers(new_out[s, f, c * half : (c + 1) * half, :]) for c in range(2)
                ]
                sides = [jnp.concatenate(pair, axis=1) for pair in zip(*parts_of)]
                rows_of[f] = ends + sides
                for e in range(6):
                    at = 6 * f + e
                    ghosts[n_new + s, at : at + 1, :] = rows_of[f][e ^ 1]

            @pl.when(has_after)
            def _(s=s, r=r):
                face_copy(1, s, r).start()

            @pl.when(has_before)
            def _(s=s, r=r):
                face_copy(0, s, r).start()

            for f in range(*r):
                for e in range(6):
                    at = 6 * f + e
                    faces[s, at : at + 1, :] = rows_of[f][e]

    every_line.wait_recv()
    total = jnp.zeros(mass_in.shape[1:], jnp.float32)
    for a in range(size_y):
        total = total + mass_in[first_line + lax.rem(iy - a + size_y, size_y)]
    total = total / float(n_old * devices * edge * face)
    for a in range(2):
        mass_out[a : a + 1, :] = total[:, 8 * a : 8 * a + fields]

    all_of(inbox, bulk_send, chip_recv.at[0]).wait_send()
    all_of(mass_in.at[: bits + size_y], mass_send, line_recv).wait_send()

    @pl.when(has_before)
    def _():
        face_copy(1, None).wait_recv()
        face_copy(0, None).wait_send()

    @pl.when(has_after)
    def _():
        face_copy(0, None).wait_recv()
        face_copy(1, None).wait_send()

    for s in range(n_new):
        ghost = jnp.zeros((tall, face), jnp.float32)
        present = jnp.zeros((tall, face), jnp.int32)
        for e in range(6):
            side = side_ref[s, e]
            source = linear + side - 1
            here = (side < 3) & (source >= 0) & (source < devices)
            place = jnp.where(side < 3, side, 0) * n_new + patch_ref[s, e]
            ghost = jnp.where(which == e, ghosts[place], ghost)
            present = jnp.where(which == e, here.astype(jnp.int32), present)
        jump = jnp.where(present > 0, ghost - faces[s], 0.0)
        for f in range(fields):
            jump_out[s, f] = jump[6 * f : 6 * f + 6]


def write_out(*refs):
    sems = refs[-1]
    copies = [pltpu.make_async_copy(refs[i], refs[3 + i], sems.at[i]) for i in range(3)]
    for copy in copies:
        copy.start()
    for copy in copies:
        copy.wait()


def body(
    old_data, pair_old, pair_slot, pair_shift, pair_dest, new_ratio, neighbor_side, neighbor_patch
):
    n_old, fields, edge, face = old_data.shape
    n_pairs = pair_old.shape[0]
    n_new = neighbor_side.shape[0]
    size_x, size_y, size_z = (lax.axis_size(a) for a in AXES)
    chips = size_x * size_z // 2
    assert size_z % 2 == 0 and chips & (chips - 1) == 0
    half = edge // 2
    bits = chips.bit_length() - 1
    tall = -(-6 * fields // 8) * 8
    dims = (size_x, size_y, size_z, n_old, n_new, n_pairs, fields, edge)
    f32 = jnp.float32
    vmem = pl.BlockSpec(memory_space=pltpu.VMEM)
    tables = (pair_old, pair_slot, pair_shift.T, pair_dest.reshape(n_pairs))
    tables += (new_ratio, neighbor_side, neighbor_patch)
    dma = pltpu.SemaphoreType.DMA
    shapes = ((n_new, fields, edge, face), (n_new, fields, 6, face), (2, fields))
    results = pl.pallas_call(
        functools.partial(kernel, dims),
        out_shape=tuple(pltpu.VMEM(s, f32) for s in shapes),
        in_specs=[pl.BlockSpec(memory_space=pl.ANY)] * 8,
        out_specs=(vmem, vmem, vmem),
        scratch_shapes=[pltpu.SMEM(t.shape, jnp.int32) for t in tables]
        + [
            pltpu.VMEM((2, face, face), jnp.int32),
            pltpu.VMEM((2, fields * edge, 2 * fields * edge), jnp.int32),
            pltpu.VMEM((n_old, fields, edge, face), f32),
            pltpu.VMEM((n_pairs + 1, 2, fields, half, face), f32),
            pltpu.VMEM((chips, 2, n_new, fields, half, face), f32),
            pltpu.VMEM((chips, 2, n_new, fields, half, face), f32),
            pltpu.VMEM((2 * chips - 1, 2, n_new, fields, half, face), f32),
            pltpu.VMEM((n_new, tall, face), f32),
            pltpu.VMEM((3 * n_new, tall, face), f32),
            pltpu.VMEM((bits + 2, 1, 128), f32),
            pltpu.VMEM((bits + 1 + size_y, 1, 128), f32),
            dma,
            dma((len(tables),)),
            pltpu.SemaphoreType.REGULAR,
            pltpu.SemaphoreType.REGULAR((bits,)),
            pltpu.SemaphoreType.REGULAR,
            dma,
            dma((n_new + chips - 1,)),
            dma((len(plan_of(bits, n_new, fields)[1]),)),
            dma((2,)),
            dma((2,)),
            dma,
            dma((bits + 1,)),
            dma,
        ],
        compiler_params=pltpu.CompilerParams(collective_id=0, has_side_effects=True),
    )(old_data, *tables)
    return pl.pallas_call(
        write_out,
        out_shape=tuple(jax.ShapeDtypeStruct(s, f32) for s in shapes),
        in_specs=[vmem] * 3,
        out_specs=(pl.BlockSpec(memory_space=pl.ANY),) * 3,
        scratch_shapes=[dma((3,))],
    )(*(pltpu.with_memory_space_constraint(r, pltpu.VMEM) for r in results))


def solution(mesh):
    whole = P(AXES)
    return jax.shard_map(
        body,
        mesh=mesh,
        in_specs=(whole, whole, whole, whole, whole, P(), whole, whole),
        out_specs=(whole, whole, P()),
        check_vma=False,
    )
```
